32 devices in a mesh: gx: 2 (over y), gy: 4 (over x, core), gz: 4 (over z).
Axes of the slice: x: 2, y: 2, z: 4, core: 2. Of those that a mesh axis runs over, the one named last changes fastest.
Arguments:
- probe_bits: int32 [8, 32, 512], P('gx', 'gz', 'gy'), may hold values from -2147483648 to 2147483646
- disorder_levels: int32 [8, 32, 512], P('gx', 'gz', 'gy'), may hold values from -2147483648 to 2147483647, as said below
Outputs:
- moments: float32 [3, 8], replicated
- previous: float32 [8, 8, 128, 512], P(None, 'gx', 'gz', 'gy')
- current: float32 [8, 8, 128, 512], P(None, 'gx', 'gz', 'gy')
The draws below stay inside these ranges and needn't reach their ends.
Inputs may be any that keep to these rules, and one draw needn't show every extreme that they name: `disorder_levels`: every byte of a word is a level 0 to 255.
All inputs are finite; a program needn't handle non-finite values.
Results may differ from the reference program's by a relative error of at most 0.00002.
Values sent between devices are 32-bit elements; how exact they have to be, the bound alone decides.
A program may use at most 64 MiB of HBM per device.

```python
import jax
import jax.numpy as jnp
from jax import lax

PROBES = 8
LEVELS = 256
NX = 8
NY = 512
NZ = 128
NSITES = 524288


def draw_disorder_levels(key, part):
    shape = (NX, NZ, NY)
    group = jax.random.randint(jax.random.fold_in(key, 11), (), 0, 2)
    base = 32 + jax.random.randint(jax.random.fold_in(key, 12), (), 0, 64) + 128 * group
    slope = 32 * (2 * jax.random.randint(jax.random.fold_in(key, 13), (), 0, 2) - 1)
    offsets = jax.random.randint(jax.random.fold_in(key, 14), (4, 4, 4), -16, 17)
    widths = jax.random.randint(jax.random.fold_in(key, 15), (4, 4, 4), 16, 80)
    patch_x = lax.broadcasted_iota(jnp.int32, shape, 0) * 4 // NX
    patch_z = lax.broadcasted_iota(jnp.int32, shape, 1) * 4 // NZ
    patch_y = lax.broadcasted_iota(jnp.int32, shape, 2) * 4 // NY
    local_offset = offsets[patch_x, patch_z, patch_y]
    local_width = widths[patch_x, patch_z, patch_y]
    centre = base + slope * (patch_x - 1) + local_offset
    raw = jax.random.randint(jax.random.fold_in(key, 16), shape, 0, 161)
    jitter = raw % (2 * local_width + 1) - local_width
    patchy = jnp.clip(centre + jitter, 0, LEVELS - 1)
    background = jax.random.randint(jax.random.fold_in(key, 17), shape, 0, LEVELS)
    picker = jax.random.randint(jax.random.fold_in(key, 18), shape, 0, 8)
    levels = jnp.where(picker == 0, background, patchy).astype(jnp.int32)
    grouped = levels.reshape(NX, NZ // 4, 4, NY)
    top_byte = grouped[:, :, 3, :]
    top_signed = jnp.where(top_byte >= 128, top_byte - 256, top_byte)
    packed = grouped[:, :, 0, :] + grouped[:, :, 1, :] * 256 + grouped[:, :, 2, :] * 65536 + top_signed * 16777216
    return packed.astype(jnp.int32)


def plant(entries, rng, low, top_value):
    shape = entries.shape
    place = [jax.random.randint(jax.random.fold_in(rng, axis), (), 0, shape[axis]) for axis in range(len(shape))]
    entries = entries.at[tuple(place)].set(low)
    longest = shape.index(max(shape))
    place[longest] = (place[longest] + 1) % shape[longest]
    return entries.at[tuple(place)].set(top_value)


def shard_levels(stream_key, extent, cuts, smallest, top_value):
    factor_of, own = 1.0, jax.random.fold_in(stream_key, 6)
    for axis_at, parts in cuts:
        heights = jnp.exp(jax.random.uniform(jax.random.fold_in(own, axis_at), (parts,), jnp.float32, smallest / len(cuts), top_value / len(cuts)))
        factor_of = factor_of * jnp.repeat(heights, extent[axis_at] // parts).reshape([-1 if axis == axis_at else 1 for axis in range(len(extent))])
    return factor_of


def setup_inputs(seed: int = 0) -> dict:
    seeds = jax.random.split(jax.random.key(seed), 3)
    probe_bits = plant(jax.random.randint(seeds[0], (NX, NZ // 4, NY), -2147483648, 2147483647), jax.random.fold_in(seeds[0], 1), -2147483648, 2147483646).astype(jnp.int32)
    disorder_levels = draw_disorder_levels(jax.random.fold_in(seeds[2], 71), 0)
    return dict(probe_bits=probe_bits, disorder_levels=disorder_levels)


disorder_width = 4.0
spectral_scale = 8.4


def unpack_signs(packed):
    shifts = 4 * jnp.arange(PROBES, dtype=jnp.int32)[:, None] + jnp.arange(4, dtype=jnp.int32)[None, :]
    bit_values = jnp.right_shift(packed[None, :, :, None, :], shifts[:, None, None, :, None]) & 1
    layout = bit_values.shape
    flat = bit_values.reshape(layout[0], layout[1], layout[2] * layout[3], layout[4])
    return 2.0 * flat.astype(jnp.float32) - 1.0


def unpack_energy(packed):
    shifts = 8 * jnp.arange(4, dtype=jnp.int32)
    levels = jnp.right_shift(packed[:, :, None, :], shifts[None, None, :, None]) & 255
    layout = levels.shape
    flat = levels.reshape(layout[0], layout[1] * layout[2], layout[3])
    return disorder_width * ((flat.astype(jnp.float32) + 0.5) / LEVELS - 0.5)


def apply_ham(field, energy):
    beside = jnp.roll(field, -1, 1) + jnp.roll(field, 1, 1)
    beside = beside + jnp.roll(field, -1, 3) + jnp.roll(field, 1, 3)
    beside = beside + jnp.roll(field, -1, 2) + jnp.roll(field, 1, 2)
    return (energy[None] * field - beside) / spectral_scale


def reference(probe_bits, disorder_levels):
    signs = unpack_signs(probe_bits)
    energy = unpack_energy(disorder_levels)
    first = apply_ham(signs, energy)
    second = 2.0 * apply_ham(first, energy) - signs
    third = 2.0 * apply_ham(second, energy) - first
    moments = jnp.stack([jnp.sum(signs * vec, axis=(1, 2, 3)) for vec in (first, second, third)]) / NSITES
    return moments, second, third
```

```python
import functools

import jax
import jax.numpy as jnp
from jax import lax
from jax.experimental import pallas as pl
from jax.experimental.pallas import tpu as pltpu
from jax.sharding import PartitionSpec as P

PROBES = 8
LEVELS = 256
LANES = 128
SITES = 4
STRIP = 12

disorder_width = 4.0
spectral_scale = 8.4
MESH = pl.DeviceIdType.MESH


def kernel(names, sizes, p_hbm, d_hbm, prow_hbm, drow_hbm, mom_ref, prev_ref, cur_ref,
           p_ref, d_ref, words, packs, strips, v0, v1, v2, en, s0, s1, s2, se, accs, moms,
           load_sem, send_sem, recv_sem, msend_sem, mrecv_sem, token):
    X, W, _ = p_ref.shape
    Z = SITES * W
    nbx = packs.shape[0]
    M = nbx * X
    gx, gy, gz = sizes["gx"], sizes["gy"], sizes["gz"]
    ix, iy, iz = (lax.axis_index(a) for a in ("gx", "gy", "gz"))
    total = gx * gy * gz
    me = (ix * gy + iy) * gz + iz
    last = gz - 1
    staged = gx <= 3 and gy <= 4 and 3 <= gz <= 4

    def device(x, y, z):
        at = {"gx": x, "gy": y, "gz": z}
        return tuple(at[a] for a in names)

    loads = [pltpu.make_async_copy(src, dst, load_sem.at[n]) for n, (src, dst) in enumerate((
        (p_hbm, p_ref), (d_hbm, d_ref),
        (prow_hbm, words.at[0, pl.ds(0, X), pl.ds(1, W)]), (drow_hbm, words.at[1, pl.ds(0, X), pl.ds(1, W)])))]
    for load in loads:
        load.start()

    def around(at, size):
        steps = [at]
        for _ in range(size - 1):
            steps.append(jnp.where(steps[-1] + 1 == size, 0, steps[-1] + 1))
        return steps

    around_x, around_y = around(ix, gx), around(iy, gy)

    def plane_of_others(z, act):
        for x in range(gx):
            for y in range(gy):
                if x or y:
                    act(device(around_x[x], around_y[y], z))

    def whole_plane(z, act):
        for x in range(gx):
            for y in range(gy):
                act(device(around_x[x], around_y[y], z))

    def each_other(act):
        if gz <= 4:
            for z in around(iz, gz)[1:]:
                whole_plane(z, act)
        else:
            def step(k, _):
                whole_plane(lax.rem(iz + k, gz), act)
                return 0
            lax.fori_loop(1, gz, step, 0)
        plane_of_others(iz, act)

    xs = (0, 1) if nbx == 2 else (0, 1, -1)
    ys = (0, 1, -1)

    def at_offset(ox, oy, oz):
        return device(lax.rem(ix + ox + gx, gx), lax.rem(iy + oy + gy, gy), lax.rem(iz + oz + gz, gz))

    barrier = pltpu.get_barrier_semaphore()

    def greet(to):
        pl.semaphore_signal(barrier, inc=1, device_id=to, device_id_type=MESH)

    per_plane = len(xs) * len(ys)
    if staged:
        @pl.when(iz < last)
        def _():
            whole_plane(last, greet)
            for ox in xs:
                for oy in ys:
                    if ox or oy:
                        greet(at_offset(ox, oy, 0))

        @pl.when(iz == last)
        def _():
            plane_of_others(iz, greet)

        @pl.when(iz > 0)
        def _():
            for ox in xs:
                for oy in ys:
                    greet(at_offset(ox, oy, -1))

        @pl.when(iz + 1 < last)
        def _():
            for ox in xs:
                for oy in ys:
                    greet(at_offset(ox, oy, 1))
    else:
        each_other(greet)

    lane = lax.broadcasted_iota(jnp.int32, (2 * X, LANES), 1)
    slot_word = (lane * 10923) >> 17
    column = lane - STRIP * slot_word

    for load in loads:
        load.wait()
    pack = jnp.zeros((2 * X, LANES), jnp.int32)
    for w in range(W):
        rows = jnp.concatenate([p_ref[:, w, :], d_ref[:, w, :]], axis=0)
        base = STRIP * (w + 1)
        first = pltpu.roll(rows, (base - (LANES - 3)) % LANES, 1)
        second = pltpu.roll(rows, (base + 5 - (LANES - 2)) % LANES, 1)
        pack = jnp.where(slot_word == w + 1, jnp.where(column < 5, first, second), pack)
    packs[0, 1, 1] = pack

    if staged:
        @pl.when(iz == last)
        def _():
            pl.semaphore_wait(barrier, total - 1)

        @pl.when(iz == 0)
        def _():
            pl.semaphore_wait(barrier, 2 * per_plane - 1)

        @pl.when((iz > 0) & (iz < last))
        def _():
            pl.semaphore_wait(barrier, 3 * per_plane - 1)
    else:
        pl.semaphore_wait(barrier, total - 1)

    slot_of = {0: 0, 1: nbx - 1, -1: 1}
    groups = {"far": [], "near": [], 1: [], -1: []}
    count = 0
    for oz in (0, 1, -1):
        for ox in xs:
            for oy in ys:
                if ox == 0 and oz == 0 and oy == 0:
                    continue
                s = slot_of[ox]
                moves = []
                if oy == 0:
                    src_w, dst_w = {0: (pl.ds(1, W), pl.ds(1, W)), 1: (pl.ds(W, 1), pl.ds(0, 1)),
                                    -1: (pl.ds(1, 1), pl.ds(W + 1, 1))}[oz]
                    for f in range(2):
                        moves.append((words.at[f, pl.ds(0, X), src_w], words.at[f, pl.ds(s * X, X), dst_w]))
                moves.append((packs.at[0, 1, 1], packs.at[s, 1 - oz, 1 - oy]))
                for src, dst in moves:
                    groups[oz if oz else ("far" if ox else "near")].append(pltpu.make_async_remote_copy(
                        src_ref=src, dst_ref=dst, send_sem=send_sem.at[count], recv_sem=recv_sem.at[count],
                        device_id=at_offset(ox, oy, oz), device_id_type=MESH))
                    count += 1

    for copy in groups["far"] + groups[1] + groups["near"]:
        copy.start()
    if staged:
        @pl.when(iz > 0)
        def _():
            for copy in groups[-1]:
                copy.start()

        @pl.when(iz == last)
        def _():
            for ox in xs:
                for oy in ys:
                    pl.semaphore_signal(token, inc=1, device_id=at_offset(ox, oy, 1), device_id_type=MESH)
    else:
        for copy in groups[-1]:
            copy.start()

    scale = 1.0 / spectral_scale
    e_mul = disorder_width / LEVELS / spectral_scale
    e_add = disorder_width * (0.5 / LEVELS - 0.5) / spectral_scale
    probe = lax.broadcasted_iota(jnp.int32, (PROBES, LANES), 0)
    lane8 = lax.broadcasted_iota(jnp.int32, (PROBES, LANES), 1)
    slot8 = (lane8 * 10923) >> 17
    col8 = lane8 - STRIP * slot8
    lifts = [31 - (SITES * probe + j) for j in range(SITES)]
    zero = jnp.zeros((PROBES, LANES), jnp.float32)

    def ends(at, size):
        return at == 0, at != size - 1

    (low_x, high_x), (low_y, high_y), (low_z, high_z) = ends(ix, gx), ends(iy, gy), ends(iz, gz)

    def sign_of(row, j):
        return jnp.where((jnp.broadcast_to(row, (PROBES, LANES)) << lifts[j]) < 0, 1.0, -1.0).astype(jnp.float32)

    def energy_of(row, j):
        level = (jnp.broadcast_to(row, (PROBES, LANES)) >> (8 * j)) & 255
        return level.astype(jnp.float32) * e_mul + e_add

    def unpack(q, zs):
        for z in zs:
            w, j = divmod(z + SITES, SITES)
            v0[q, z + 3] = sign_of(words[0, q, w], j)
            en[q, z + 3] = energy_of(words[1, q, w], j)

    def plane(e):
        return lax.rem(e + M, M)

    def planes(low, high, body):
        def step(i, _):
            body(plane(i - low))
            return 0
        lax.fori_loop(0, min(M, X + low + high), step, 0)

    def join_strips(s, oz):
        return jnp.where(column < 3, packs[s, oz, 0], jnp.where(column < 7, packs[s, oz, 1], packs[s, oz, 2]))

    def unpack_strips(s):
        for x in range(X):
            for j in range(SITES):
                s0[s * X + x, j] = sign_of(strips[s, x:x + 1], j)
                se[s * X + x, j] = energy_of(strips[s, X + x:X + x + 1], j)

    def strip_sum(src, q, up, down):
        mine = [src[q, j] for j in range(SITES)]
        sums, rights, ups = [], [], []
        for j in range(SITES):
            z_up = mine[j + 1] if j + 1 < SITES else pltpu.roll(mine[0], LANES - STRIP, 1)
            z_down = mine[j - 1] if j > 0 else pltpu.roll(mine[SITES - 1], STRIP, 1)
            sums.append(src[up, j] + src[down, j] + pltpu.roll(mine[j], LANES - 1, 1)
                        + pltpu.roll(mine[j], 1, 1) + z_up + z_down)
        return mine, sums

    def edges_of(mine):
        return [jnp.where(col8 == 1, pltpu.roll(m, LANES - 6, 1), m) for m in mine]

    def site_sum(src, q, up, down, z, edges):
        w, j = divmod(z + SITES, SITES)
        fix = pltpu.roll(edges[j], (-(STRIP * w + 2)) % LANES, 1)
        mid = src[q, z + 3]
        right = jnp.where(lane8 == LANES - 1, fix, pltpu.roll(mid, LANES - 1, 1))
        left = jnp.where(lane8 == 0, fix, pltpu.roll(mid, 1, 1))
        return mid, src[up, z + 3] + src[down, z + 3] + right + left + src[q, z + 4] + src[q, z + 2]

    def around_plane(e):
        return plane(e), plane(e + 1), plane(e + M - 1)

    site_cols = ((col8 == 2) & low_y) | ((col8 == 7) & high_y)
    bond_cols = (((col8 == 1) | (col8 == 2)) & low_y) | (((col8 == 6) | (col8 == 7)) & high_y)
    lane_sites = ((lane8 > 0) | low_y) & ((lane8 < LANES - 1) | high_y)
    lane_bonds = ((lane8 > 0) | low_y) & ((lane8 < LANES - 2) | (high_y & (lane8 < LANES - 1)))

    def keep(mask, value):
        return jnp.where(mask, value, 0.0)

    def level_one(e, beside, zs, z_sites, z_bonds, site_on, bond_on, sums):
        q, up, down = around_plane(e)
        nb = plane(beside)
        mine, six = strip_sum(s0, q, up, down)
        fresh = []
        for j in range(SITES):
            fresh.append(se[q, j] * mine[j] - scale * six[j])
            s1[q, j] = fresh[j]
        edges = edges_of(mine)
        if sums is None:
            for z in zs:
                mid, total_six = site_sum(v0, q, up, down, z, edges)
                v1[q, z + 3] = en[q, z + 3] * mid - scale * total_six
            return None
        one, two, three, bond, right = zero, zero, zero, zero, zero
        t_one, t_two, t_three, t_bond = zero, zero, zero, zero
        for j in range(SITES):
            z_at = SITES * (slot8 - 1) + j
            in_sites = (z_at >= min(z_sites)) & (z_at <= max(z_sites))
            in_bonds = (z_at >= min(z_bonds)) & (z_at <= max(z_bonds))
            new = fresh[j]
            z_up = fresh[j + 1] if j + 1 < SITES else pltpu.roll(fresh[0], LANES - STRIP, 1)
            here = site_cols & in_sites
            square = new * new
            t_one = t_one + keep(here, mine[j] * new)
            t_two = t_two + keep(here, square)
            t_three = t_three + keep(here, se[q, j] * square)
            pairs = keep(site_cols & in_bonds, z_up) + keep(bond_cols & in_sites, pltpu.roll(new, LANES - 1, 1))
            t_three = t_three - (2.0 * scale) * (new * pairs)
            t_bond = t_bond + keep(here, new * s1[nb, j])
        before = None
        done = {}
        if min(z_bonds) < min(zs):
            done[min(z_bonds)] = v1[q, min(z_bonds) + 3]
        if max(z_bonds) + 1 > max(zs):
            done[max(z_bonds) + 1] = v1[q, max(z_bonds) + 4]
        for z in zs:
            mid, total_six = site_sum(v0, q, up, down, z, edges)
            energy = en[q, z + 3]
            new = energy * mid - scale * total_six
            v1[q, z + 3] = new
            if z in z_sites:
                square = new * new
                one, two, three = one + mid * new, two + square, three + energy * square
                right = right + new * pltpu.roll(new, LANES - 1, 1)
                bond = bond + new * v1[nb, z + 3]
            done[z] = new
            for at in (z - 1, z):
                if at in z_bonds and at in done and at + 1 in done:
                    three = three - (2.0 * scale) * (done[at] * done[at + 1])
        parts = (keep(lane_sites, one) + t_one, keep(lane_sites, two) + t_two,
                 keep(lane_sites, three) + t_three - (2.0 * scale) * keep(lane_bonds, right))
        bond = (-2.0 * scale) * (keep(lane_sites, bond) + t_bond)
        parts = tuple(jnp.where(site_on, part, 0.0) for part in parts)
        bond = jnp.where(bond_on, bond, 0.0)
        return sums[0] + parts[0], sums[1] + parts[1], sums[2] + parts[2] + bond

    def inner_planes(zs, z_sites, z_bonds, sums):
        def body(e, sums):
            return level_one(e, e - 1, zs, z_sites, z_bonds, True, e > 1, sums)
        return lax.fori_loop(1, X - 1, body, sums)

    def outer_planes(zs, z_sites, z_bonds, sums):
        def body(i, sums):
            step = lax.rem(i, 3)
            upward = i < 3
            e = jnp.where(upward, X - 1 + step, -step)
            on = (upward & high_x) | (jnp.logical_not(upward) & low_x)
            return level_one(e, jnp.where(upward, e - 1, e + 1), zs, z_sites, z_bonds, on & (step < 2), on, sums)
        return lax.fori_loop(0, 6, body, sums)

    def level_two(e, zs):
        q, up, down = around_plane(e)
        mine, sums = strip_sum(s1, q, up, down)
        for j in range(SITES):
            s2[q, j] = 2.0 * (se[q, j] * mine[j] - scale * sums[j]) - s0[q, j]
        edges = edges_of(mine)
        for z in zs:
            mid, total_six = site_sum(v1, q, up, down, z, edges)
            v2[q, z + 3] = 2.0 * (en[q, z + 3] * mid - scale * total_six) - v0[q, z + 3]

    def level_three(x, zs):
        q, up, down = around_plane(x)
        edges = edges_of([s2[q, j] for j in range(SITES)])
        for z in zs:
            mid, total_six = site_sum(v2, q, up, down, z, edges)
            new = 2.0 * (en[q, z + 3] * mid - scale * total_six) - v1[q, z + 3]
            at = pl.ds(x * Z + z, PROBES, stride=X * Z)
            prev_ref[at, :] = mid
            cur_ref[at, :] = new

    def levels_two_three(twos, threes):
        def two(i, _):
            level_two(i - 1, twos)
            return 0

        def three(x, _):
            level_three(x, threes)
            return 0

        lax.fori_loop(0, X + 2, two, 0)
        lax.fori_loop(0, X, three, 0)

    def send_moments(sums):
        row = zero
        for n, acc in enumerate(sums):
            summed = jnp.broadcast_to(jnp.sum(acc, axis=1, keepdims=True), (PROBES, LANES))
            row = row + jnp.where(lane8 == PROBES * n + probe, summed, 0.0)
        moms[me] = jnp.sum(row, axis=0, keepdims=True)
        each_other(lambda to: pltpu.make_async_remote_copy(
            src_ref=moms.at[me], dst_ref=moms.at[me], send_sem=msend_sem, recv_sem=mrecv_sem,
            device_id=to, device_id_type=MESH).start())

    def unpack_own(x, _):
        unpack(x, range(Z))
        return 0

    def unpack_far(i, _):
        unpack(plane(X + i), range(Z))
        return 0

    def unpack_low(i, _):
        unpack(plane(i - 3), range(Z))
        return 0

    lax.fori_loop(0, X, unpack_own, 0)
    for copy in groups["near"]:
        copy.wait_recv()
    strips[0] = join_strips(0, 1)
    unpack_strips(0)
    main = range(1, Z - 1)
    sums = inner_planes(main, main, range(1, Z - 2), (zero, zero, zero))
    for copy in groups["far"]:
        copy.wait_recv()
    for s in range(1, nbx):
        strips[s] = join_strips(s, 1)
        unpack_strips(s)
    if M <= X + 6:
        lax.fori_loop(0, M - X, unpack_far, 0)
    else:
        lax.fori_loop(0, 3, unpack_far, 0)
        lax.fori_loop(0, 3, unpack_low, 0)
    sums = outer_planes(main, main, range(1, Z - 2), sums)
    for n in range(3):
        accs[n] = sums[n]

    @pl.when(iz == last)
    def _():
        send_moments([accs[n] for n in range(3)])

    levels_two_three(range(2, Z - 2), range(3, Z - 3))

    if staged:
        @pl.when(iz == 0)
        def _():
            pl.semaphore_wait(token, per_plane)
            for copy in groups[-1]:
                copy.start()

    def side(up):
        for copy in groups[-1 if up else 1]:
            copy.wait_recv()
        outside = range(Z, Z + 3) if up else range(-3, 0)
        planes(3, 3, lambda q: unpack(q, outside))
        for s in range(nbx):
            if up:
                strips[s] = jnp.where(slot_word == W + 1, pltpu.roll(join_strips(s, 2), (STRIP * W) % LANES, 1), strips[s])
            else:
                strips[s] = jnp.where(slot_word == 0, pltpu.roll(join_strips(s, 0), (-STRIP * W) % LANES, 1), strips[s])
            unpack_strips(s)
        if up:
            ones, z_sites, z_bonds = range(Z - 1, Z + 2), range(Z - 1, Z + 1), range(Z - 2, Z + 1)
            twos, threes = range(Z - 2, Z + 1), range(Z - 3, Z)
        else:
            ones, z_sites, z_bonds = range(-2, 1), range(-1, 1), range(-2, 1)
            twos, threes = range(-1, 2), range(0, 3)
        sums = inner_planes(ones, z_sites, z_bonds, (zero, zero, zero))
        sums = outer_planes(ones, z_sites, z_bonds, sums)
        on = high_z if up else low_z
        for n in range(3):
            accs[n] = accs[n] + jnp.where(on, sums[n], 0.0)

        if up:
            @pl.when((iz > 0) & (iz < last))
            def _():
                send_moments([accs[n] for n in range(3)])
        else:
            @pl.when(iz == 0)
            def _():
                send_moments([accs[n] for n in range(3)])
        levels_two_three(twos, threes)

    @pl.when(iz == last)
    def _():
        side(False)

    side(True)

    @pl.when(iz < last)
    def _():
        side(False)

    others = moms.at[pl.ds(0, total - 1)]
    pltpu.make_async_copy(others, others, mrecv_sem).wait()
    sites = total * X * Z * LANES
    sums = jnp.sum(moms[...], axis=0) * (1.0 / sites)
    first = sums
    second = 2.0 * pltpu.roll(sums, LANES - PROBES, 1) - 1.0
    third = 4.0 * pltpu.roll(sums, LANES - 2 * PROBES, 1) - 3.0 * sums
    mom_ref[...] = jnp.concatenate([first, second, third], axis=0)[:, :PROBES]
    pltpu.make_async_copy(others, others, msend_sem).wait()
    for group in groups.values():
        for copy in group:
            copy.wait_send()


def write_out(mom_ref, prev_ref, cur_ref, mom_hbm, prev_hbm, cur_hbm, sem):
    copies = [pltpu.make_async_copy(src, dst, sem.at[n]) for n, (src, dst) in enumerate((
        (prev_ref, prev_hbm), (cur_ref, cur_hbm), (mom_ref, mom_hbm)))]
    for copy in copies:
        copy.start()
    for copy in copies:
        copy.wait()


def per_device(names, sizes, probe_bits, disorder_levels):
    X, W, Y = probe_bits.shape
    if Y != LANES or STRIP * (W + 2) > LANES or X < 3:
        raise ValueError("block size")
    Z = SITES * W
    nbx = 2 if sizes["gx"] == 2 else 3
    M = nbx * X
    n_copies = (9 * nbx - 1) + 2 * (3 * nbx - 1)
    total = sizes["gx"] * sizes["gy"] * sizes["gz"]
    rows = (X, W, 1, Y)
    vmem = pl.BlockSpec(memory_space=pltpu.VMEM)
    f32, i32 = jnp.float32, jnp.int32
    tile = (PROBES, LANES)
    hbm = pl.BlockSpec(memory_space=pltpu.HBM)
    out_shape = (
        jax.ShapeDtypeStruct((3, PROBES), f32),
        jax.ShapeDtypeStruct((PROBES * X * Z, Y), f32),
        jax.ShapeDtypeStruct((PROBES * X * Z, Y), f32),
    )
    results = pl.pallas_call(
        functools.partial(kernel, names, sizes),
        out_shape=out_shape,
        in_specs=[hbm] * 4,
        out_specs=(vmem,) * 3,
        scratch_shapes=[
            pltpu.VMEM((X, W, Y), i32),
            pltpu.VMEM((X, W, Y), i32),
            pltpu.VMEM((2, M, W + 2, 1, LANES), i32),
            pltpu.VMEM((nbx, 3, 3, 2 * X, LANES), i32),
            pltpu.VMEM((nbx, 2 * X, LANES), i32),
            pltpu.VMEM((M, Z + 6) + tile, f32),
            pltpu.VMEM((M, Z + 6) + tile, f32),
            pltpu.VMEM((M, Z + 6) + tile, f32),
            pltpu.VMEM((M, Z + 6) + tile, f32),
            pltpu.VMEM((M, SITES) + tile, f32),
            pltpu.VMEM((M, SITES) + tile, f32),
            pltpu.VMEM((M, SITES) + tile, f32),
            pltpu.VMEM((M, SITES) + tile, f32),
            pltpu.VMEM((3,) + tile, f32),
            pltpu.VMEM((total, 1, LANES), f32),
            pltpu.SemaphoreType.DMA((4,)),
            pltpu.SemaphoreType.DMA((n_copies,)),
            pltpu.SemaphoreType.DMA((n_copies,)),
            pltpu.SemaphoreType.DMA,
            pltpu.SemaphoreType.DMA,
            pltpu.SemaphoreType.REGULAR,
        ],
        compiler_params=pltpu.CompilerParams(collective_id=0, has_side_effects=True,
                                             vmem_limit_bytes=40 * 1024 * 1024),
    )(*[pltpu.with_memory_space_constraint(a, pltpu.HBM) for a in (probe_bits, disorder_levels, probe_bits.reshape(rows), disorder_levels.reshape(rows))])
    moments, previous, current = pl.pallas_call(
        write_out,
        out_shape=out_shape,
        in_specs=[vmem] * 3,
        out_specs=(hbm,) * 3,
        scratch_shapes=[pltpu.SemaphoreType.DMA((3,))],
        compiler_params=pltpu.CompilerParams(vmem_limit_bytes=16 * 1024 * 1024),
    )(*results)
    shape = (PROBES, X, Z, Y)
    return moments, previous.reshape(shape), current.reshape(shape)


def solution(mesh):
    placed = (P("gx", "gz", "gy"), P("gx", "gz", "gy"))
    sizes = {a: mesh.shape[a] for a in mesh.axis_names}
    return jax.shard_map(
        functools.partial(per_device, tuple(mesh.axis_names), sizes),
        mesh=mesh,
        in_specs=placed,
        out_specs=(P(), P(None, "gx", "gz", "gy"), P(None, "gx", "gz", "gy")),
        check_vma=False,
    )
```

```python
import functools

import jax
import jax.numpy as jnp
from jax import lax
from jax.experimental import pallas as pl
from jax.experimental.pallas import tpu as pltpu
from jax.sharding import PartitionSpec as P

PROBES = 8
LEVELS = 256
LANES = 128
SITES = 4
STRIP = 12
PAD = 4

disorder_width = 4.0
spectral_scale = 8.4
MESH = pl.DeviceIdType.MESH


def kernel(names, sizes, p_hbm, d_hbm, prow_hbm, drow_hbm, mom_ref, prev_ref, cur_ref,
           p_ref, d_ref, words, packs, strips, v0, v1, v2, en, s0, s1, s2, se, accs, moms,
           load_sem, send_sem, recv_sem, msend_sem, mrecv_sem, above, entered):
    X, W, _ = p_ref.shape
    Z = SITES * W
    nbx = packs.shape[0]
    M = nbx * X
    gx, gy, gz = sizes["gx"], sizes["gy"], sizes["gz"]
    ix, iy, iz = (lax.axis_index(a) for a in ("gx", "gy", "gz"))
    total = gx * gy * gz
    me = (ix * gy + iy) * gz + iz
    last = gz - 1
    staged = gx <= 3 and gy <= 4 and 3 <= gz <= 4

    def device(x, y, z):
        at = {"gx": x, "gy": y, "gz": z}
        return tuple(at[a] for a in names)

    loads = [pltpu.make_async_copy(src, dst, load_sem.at[n]) for n, (src, dst) in enumerate((
        (p_hbm, p_ref), (d_hbm, d_ref),
        (prow_hbm, words.at[0, pl.ds(0, X), pl.ds(1, W)]), (drow_hbm, words.at[1, pl.ds(0, X), pl.ds(1, W)])))]
    for load in loads:
        load.start()

    def around(at, size):
        steps = [at]
        for _ in range(size - 1):
            steps.append(jnp.where(steps[-1] + 1 == size, 0, steps[-1] + 1))
        return steps

    around_x, around_y = around(ix, gx), around(iy, gy)

    def plane_of_others(z, act):
        for x in range(gx):
            for y in range(gy):
                if x or y:
                    act(device(around_x[x], around_y[y], z))

    def whole_plane(z, act):
        for x in range(gx):
            for y in range(gy):
                act(device(around_x[x], around_y[y], z))

    def each_other(act):
        if gz <= 4:
            for z in range(gz):
                @pl.when(iz != z)
                def _(z=z):
                    whole_plane(z, act)
        else:
            def step(n, _):
                whole_plane(lax.rem(iz + n, gz), act)
                return 0
            lax.fori_loop(1, gz, step, 0)
        plane_of_others(iz, act)

    xs = (0, 1) if nbx == 2 else (0, 1, -1)
    ys = (0, 1, -1)

    def at_offset(ox, oy, oz):
        return device(lax.rem(ix + ox + gx, gx), lax.rem(iy + oy + gy, gy), lax.rem(iz + oz + gz, gz))

    barrier = pltpu.get_barrier_semaphore()

    def greet(to):
        pl.semaphore_signal(barrier, inc=1, device_id=to, device_id_type=MESH)

    per_plane = len(xs) * len(ys)
    if staged:
        @pl.when(iz < last)
        def _():
            whole_plane(last, greet)
            for ox in xs:
                for oy in ys:
                    if ox or oy:
                        greet(at_offset(ox, oy, 0))

        @pl.when(iz == last)
        def _():
            plane_of_others(iz, greet)

        @pl.when(iz + 1 < last)
        def _():
            for ox in xs:
                for oy in ys:
                    greet(at_offset(ox, oy, 1))
    else:
        each_other(greet)

    lane = lax.broadcasted_iota(jnp.int32, (2 * X, LANES), 1)
    slot_word = (lane * 10923) >> 17
    column = lane - STRIP * slot_word

    for load in loads:
        load.wait()
    pack = jnp.zeros((2 * X, LANES), jnp.int32)
    for w in range(W):
        rows = jnp.concatenate([p_ref[:, w, :], d_ref[:, w, :]], axis=0)
        base = STRIP * (w + 1)
        first = pltpu.roll(rows, (base - (LANES - 3)) % LANES, 1)
        second = pltpu.roll(rows, (base + 5 - (LANES - 2)) % LANES, 1)
        pack = jnp.where(slot_word == w + 1, jnp.where(column < 5, first, second), pack)
    packs[0, 1, 1] = pack

    if staged:
        @pl.when(iz == last)
        def _():
            pl.semaphore_wait(barrier, total - 1)

        @pl.when(iz == 0)
        def _():
            pl.semaphore_wait(barrier, per_plane - 1)

        @pl.when((iz > 0) & (iz < last))
        def _():
            pl.semaphore_wait(barrier, 2 * per_plane - 1)
    else:
        pl.semaphore_wait(barrier, total - 1)

    slot_of = {0: 0, 1: nbx - 1, -1: 1}
    groups = {"far": [], "near": [], 1: [], -1: []}
    count = 0
    for oz in (0, 1, -1):
        for ox in xs:
            for oy in ys:
                if ox == 0 and oz == 0 and oy == 0:
                    continue
                s = slot_of[ox]
                moves = []
                if oy == 0:
                    src_w, dst_w = {0: (pl.ds(1, W), pl.ds(1, W)), 1: (pl.ds(W, 1), pl.ds(0, 1)),
                                    -1: (pl.ds(1, 1), pl.ds(W + 1, 1))}[oz]
                    for f in range(2):
                        moves.append((words.at[f, pl.ds(0, X), src_w], words.at[f, pl.ds(s * X, X), dst_w]))
                moves.append((packs.at[0, 1, 1], packs.at[s, 1 - oz, 1 - oy]))
                for src, dst in moves:
                    groups[oz if oz else ("far" if ox else "near")].append(pltpu.make_async_remote_copy(
                        src_ref=src, dst_ref=dst, send_sem=send_sem.at[count], recv_sem=recv_sem.at[count],
                        device_id=at_offset(ox, oy, oz), device_id_type=MESH))
                    count += 1

    def start(copies):
        for copy in copies:
            copy.start()

    def tell(semaphore, to):
        pl.semaphore_signal(semaphore, inc=1, device_id=to, device_id_type=MESH)

    if staged:
        @pl.when(iz == last)
        def _():
            start(groups[1])

        start(groups["far"] + groups["near"])

        @pl.when(iz > 0)
        def _():
            start(groups[-1])
            for ox in xs:
                for oy in ys:
                    tell(above, at_offset(ox, oy, -1))

        @pl.when(iz == last)
        def _():
            for z in range(last):
                tell(entered, device(ix, iy, z))
    else:
        start(groups[1] + groups["far"] + groups["near"] + groups[-1])

    e_mul = disorder_width / LEVELS
    e_add = disorder_width * (0.5 / LEVELS - 0.5)
    two_mul = 2.0 / (spectral_scale * spectral_scale)
    three_mul = 2.0 / spectral_scale
    one_mul = 1.0 / spectral_scale
    probe = lax.broadcasted_iota(jnp.int32, (PROBES, LANES), 0)
    lane8 = lax.broadcasted_iota(jnp.int32, (PROBES, LANES), 1)
    slot8 = (lane8 * 10923) >> 17
    col8 = lane8 - STRIP * slot8
    lifts = [31 - (SITES * probe + j) for j in range(SITES)]
    zero = jnp.zeros((PROBES, LANES), jnp.float32)

    def sign_of(row, j):
        return jnp.where((jnp.broadcast_to(row, (PROBES, LANES)) << lifts[j]) < 0, 1.0, -1.0).astype(jnp.float32)

    def energy_of(row, j):
        level = (jnp.broadcast_to(row, (PROBES, LANES)) >> (8 * j)) & 255
        return level.astype(jnp.float32) * e_mul + e_add

    def unpack(q, zs):
        for z in zs:
            w, j = divmod(z + SITES, SITES)
            v0[q, z + SITES] = sign_of(words[0, q, w], j)
            en[q, z + SITES] = energy_of(words[1, q, w], j)

    def plane(e):
        return lax.rem(e + M, M)

    def planes(low, high, body):
        def step(i, _):
            body(plane(i - low))
            return 0
        lax.fori_loop(0, min(M, X + low + high), step, 0)

    def join_strips(s, oz):
        return jnp.where(column < 3, packs[s, oz, 0], jnp.where(column < 7, packs[s, oz, 1], packs[s, oz, 2]))

    def unpack_strips(s):
        for x in range(X):
            for j in range(SITES):
                s0[s * X + x, j] = sign_of(strips[s, x:x + 1], j)
                se[s * X + x, j] = energy_of(strips[s, X + x:X + x + 1], j)

    def strip_sum(src, q, up, down):
        mine = [src[q, j] for j in range(SITES)]
        sums, rights, ups = [], [], []
        for j in range(SITES):
            z_up = mine[j + 1] if j + 1 < SITES else pltpu.roll(mine[0], LANES - STRIP, 1)
            z_down = mine[j - 1] if j > 0 else pltpu.roll(mine[SITES - 1], STRIP, 1)
            sums.append(src[up, j] + src[down, j] + pltpu.roll(mine[j], LANES - 1, 1)
                        + pltpu.roll(mine[j], 1, 1) + z_up + z_down)
        return mine, sums

    def edges_of(mine):
        return [jnp.where(col8 == 1, pltpu.roll(m, LANES - 6, 1), m) for m in mine]

    def site_sum(src, q, up, down, z, edges):
        w, j = divmod(z + SITES, SITES)
        fix = pltpu.roll(edges[j], (-(STRIP * w + 2)) % LANES, 1)
        mid = src[q, z + SITES]
        right = jnp.where(lane8 == LANES - 1, fix, pltpu.roll(mid, LANES - 1, 1))
        left = jnp.where(lane8 == 0, fix, pltpu.roll(mid, 1, 1))
        return mid, src[up, z + SITES] + src[down, z + SITES] + right + left + src[q, z + SITES + 1] + src[q, z + SITES - 1]

    def around_plane(e):
        return plane(e), plane(e + 1), plane(e + M - 1)

    def level_one(e, zs):
        q, up, down = around_plane(e)
        mine, six = strip_sum(s0, q, up, down)
        for j in range(SITES):
            s1[q, j] = se[q, j] * mine[j] - six[j]
        edges = edges_of(mine)
        for z in zs:
            mid, total_six = site_sum(v0, q, up, down, z, edges)
            v1[q, z + SITES] = en[q, z + SITES] * mid - total_six

    def level_two(e, zs, sums):
        q, up, down = around_plane(e)
        edges = edges_of([s1[q, j] for j in range(SITES)])
        for z in zs:
            mid, total_six = site_sum(v1, q, up, down, z, edges)
            start = v0[q, z + SITES]
            new = two_mul * (en[q, z + SITES] * mid - total_six) - start
            v2[q, z + SITES] = new
            if sums is not None:
                sums = sums[0] + start * mid, sums[1] + mid * mid, sums[2] + mid * new
        return sums

    def strip_two(x, _):
        q, up, down = around_plane(x)
        mine, six = strip_sum(s1, q, up, down)
        for j in range(SITES):
            s2[q, j] = two_mul * (se[q, j] * mine[j] - six[j]) - s0[q, j]
        return 0

    def level_three(x, zs):
        q, up, down = around_plane(x)
        edges = edges_of([s2[q, j] for j in range(SITES)])
        for z in zs:
            mid, total_six = site_sum(v2, q, up, down, z, edges)
            new = three_mul * (en[q, z + SITES] * mid - total_six) - one_mul * v1[q, z + SITES]
            at = pl.ds(x * Z + z, PROBES, stride=X * Z + PAD)
            prev_ref[at, :] = mid
            cur_ref[at, :] = new

    def loop(low, high, body):
        def step(i, _):
            body(i)
            return 0
        lax.fori_loop(low, high, step, 0)

    def own_two(zs):
        return lax.fori_loop(0, X, lambda x, sums: level_two(x, zs, sums), (zero, zero, zero))

    def send_moments(sums):
        row = zero
        for n, acc in enumerate(sums):
            summed = jnp.broadcast_to(jnp.sum(acc, axis=1, keepdims=True), (PROBES, LANES))
            row = row + jnp.where(lane8 == PROBES * n + probe, summed, 0.0)
        moms[me] = jnp.sum(row, axis=0, keepdims=True)
        each_other(lambda to: pltpu.make_async_remote_copy(
            src_ref=moms.at[me], dst_ref=moms.at[me], send_sem=msend_sem, recv_sem=mrecv_sem,
            device_id=to, device_id_type=MESH).start())

    def unpack_own(x, _):
        unpack(x, range(Z))
        return 0

    def unpack_far(i, _):
        unpack(plane(X + i), range(Z))
        return 0

    def unpack_low(i, _):
        unpack(plane(i - 3), range(Z))
        return 0

    lax.fori_loop(0, X, unpack_own, 0)
    for copy in groups["near"]:
        copy.wait_recv()
    strips[0] = join_strips(0, 1)
    unpack_strips(0)
    main = range(1, Z - 1)
    loop(1, X - 1, lambda x: level_one(x, main))
    for copy in groups["far"]:
        copy.wait_recv()
    for s in range(1, nbx):
        strips[s] = join_strips(s, 1)
        unpack_strips(s)
    if M <= X + 6:
        lax.fori_loop(0, M - X, unpack_far, 0)
    else:
        lax.fori_loop(0, 3, unpack_far, 0)
        lax.fori_loop(0, 3, unpack_low, 0)

    if staged:
        @pl.when(iz < last)
        def _():
            pl.semaphore_wait(above, per_plane)
            start(groups[1])

    def ends_of(low):
        width = X - 1 - 2 * low

        def body(i):
            level_one(low + i * width, main)
        return body

    loop(0, 2, ends_of(0))
    loop(0, 2, ends_of(-1))
    sums = own_two(range(2, Z - 2))
    for n in range(3):
        accs[n] = sums[n]

    @pl.when(iz == last)
    def _():
        send_moments([accs[n] for n in range(3)])

    loop(0, min(M, X + 4) - (X + 2), ends_of(-2))

    def side(up):
        for copy in groups[-1 if up else 1]:
            copy.wait_recv()
        outside = range(Z, Z + SITES) if up else range(-SITES, 0)
        planes(3, 3, lambda q: unpack(q, outside))
        for s in range(nbx):
            if up:
                strips[s] = jnp.where(slot_word == W + 1, pltpu.roll(join_strips(s, 2), (STRIP * W) % LANES, 1), strips[s])
            else:
                strips[s] = jnp.where(slot_word == 0, pltpu.roll(join_strips(s, 0), (-STRIP * W) % LANES, 1), strips[s])
            unpack_strips(s)
        ones = range(Z - 1, Z + 3) if up else range(-3, 1)
        twos = range(Z - 2, Z + 2) if up else range(-2, 2)
        loop(0, min(M, X + 4), lambda i: level_one(i - 2, ones))
        sums = own_two(twos)
        on = (iz != last) if up else (iz == 0)
        for n in range(3):
            accs[n] = accs[n] + jnp.where(on, sums[n], 0.0)

        if up:
            @pl.when((iz > 0) & (iz < last))
            def _():
                if staged:
                    pl.semaphore_wait(entered, 1)
                send_moments([accs[n] for n in range(3)])

            @pl.when(iz == 0)
            def _():
                if staged:
                    pl.semaphore_wait(entered, 1)
                    start(groups[-1])
        else:
            @pl.when(iz == 0)
            def _():
                send_moments([accs[n] for n in range(3)])

    @pl.when(iz == last)
    def _():
        side(False)

    side(True)

    @pl.when(iz < last)
    def _():
        side(False)

    loop(0, 2, lambda i: level_two(i * (X + 1) - 1, range(Z), None))
    lax.fori_loop(0, X, strip_two, 0)
    loop(0, X, lambda x: level_three(x, range(Z)))

    others = moms.at[pl.ds(0, total - 1)]
    pltpu.make_async_copy(others, others, mrecv_sem).wait()
    sites = total * X * Z * LANES
    sums = jnp.sum(moms[...], axis=0) * (1.0 / sites)
    first = one_mul * sums
    second = two_mul * pltpu.roll(sums, LANES - PROBES, 1) - 1.0
    third = three_mul * pltpu.roll(sums, LANES - 2 * PROBES, 1) - first
    mom_ref[...] = jnp.concatenate([first, second, third], axis=0)[:, :PROBES]
    pltpu.make_async_copy(others, others, msend_sem).wait()
    for group in groups.values():
        for copy in group:
            copy.wait_send()


def write_out(mom_ref, prev_ref, cur_ref, mom_hbm, prev_hbm, cur_hbm, sem):
    rows = prev_hbm.shape[0] // PROBES
    copies = [pltpu.make_async_copy(mom_ref, mom_hbm, sem.at[2 * PROBES])]
    for n, (src, dst) in enumerate(((prev_ref, prev_hbm), (cur_ref, cur_hbm))):
        for r in range(PROBES):
            copies.append(pltpu.make_async_copy(
                src.at[pl.ds(r * (rows + PAD), rows)], dst.at[pl.ds(r * rows, rows)], sem.at[n * PROBES + r]))
    for copy in copies:
        copy.start()
    for copy in copies:
        copy.wait()


def per_device(names, sizes, probe_bits, disorder_levels):
    X, W, Y = probe_bits.shape
    if Y != LANES or STRIP * (W + 2) > LANES or X < 3:
        raise ValueError("block size")
    Z = SITES * W
    nbx = 2 if sizes["gx"] == 2 else 3
    M = nbx * X
    n_copies = (9 * nbx - 1) + 2 * (3 * nbx - 1)
    total = sizes["gx"] * sizes["gy"] * sizes["gz"]
    rows = (X, W, 1, Y)
    vmem = pl.BlockSpec(memory_space=pltpu.VMEM)
    f32, i32 = jnp.float32, jnp.int32
    tile = (PROBES, LANES)
    hbm = pl.BlockSpec(memory_space=pltpu.HBM)
    out_shape = (
        jax.ShapeDtypeStruct((3, PROBES), f32),
        jax.ShapeDtypeStruct((PROBES * X * Z, Y), f32),
        jax.ShapeDtypeStruct((PROBES * X * Z, Y), f32),
    )
    padded = jax.ShapeDtypeStruct((PROBES * (X * Z + PAD), Y), f32)
    padded_shape = (out_shape[0], padded, padded)
    results = pl.pallas_call(
        functools.partial(kernel, names, sizes),
        out_shape=padded_shape,
        in_specs=[hbm] * 4,
        out_specs=(vmem,) * 3,
        scratch_shapes=[
            pltpu.VMEM((X, W, Y), i32),
            pltpu.VMEM((X, W, Y), i32),
            pltpu.VMEM((2, M, W + 2, 1, LANES), i32),
            pltpu.VMEM((nbx, 3, 3, 2 * X, LANES), i32),
            pltpu.VMEM((nbx, 2 * X, LANES), i32),
            pltpu.VMEM((M, Z + 2 * SITES) + tile, f32),
            pltpu.VMEM((M, Z + 2 * SITES) + tile, f32),
            pltpu.VMEM((M, Z + 2 * SITES) + tile, f32),
            pltpu.VMEM((M, Z + 2 * SITES) + tile, f32),
            pltpu.VMEM((M, SITES) + tile, f32),
            pltpu.VMEM((M, SITES) + tile, f32),
            pltpu.VMEM((M, SITES) + tile, f32),
            pltpu.VMEM((M, SITES) + tile, f32),
            pltpu.VMEM((3,) + tile, f32),
            pltpu.VMEM((total, 1, LANES), f32),
            pltpu.SemaphoreType.DMA((4,)),
            pltpu.SemaphoreType.DMA((n_copies,)),
            pltpu.SemaphoreType.DMA((n_copies,)),
            pltpu.SemaphoreType.DMA,
            pltpu.SemaphoreType.DMA,
            pltpu.SemaphoreType.REGULAR,
            pltpu.SemaphoreType.REGULAR,
        ],
        compiler_params=pltpu.CompilerParams(collective_id=0, has_side_effects=True,
                                             vmem_limit_bytes=40 * 1024 * 1024),
    )(*[pltpu.with_memory_space_constraint(a, pltpu.HBM) for a in (probe_bits, disorder_levels, probe_bits.reshape(rows), disorder_levels.reshape(rows))])
    moments, previous, current = pl.pallas_call(
        write_out,
        out_shape=out_shape,
        in_specs=[vmem] * 3,
        out_specs=(hbm,) * 3,
        scratch_shapes=[pltpu.SemaphoreType.DMA((2 * PROBES + 1,))],
        compiler_params=pltpu.CompilerParams(vmem_limit_bytes=16 * 1024 * 1024),
    )(*results)
    shape = (PROBES, X, Z, Y)
    return moments, previous.reshape(shape), current.reshape(shape)


def solution(mesh):
    placed = (P("gx", "gz", "gy"), P("gx", "gz", "gy"))
    sizes = {a: mesh.shape[a] for a in mesh.axis_names}
    return jax.shard_map(
        functools.partial(per_device, tuple(mesh.axis_names), sizes),
        mesh=mesh,
        in_specs=placed,
        out_specs=(P(), P(None, "gx", "gz", "gy"), P(None, "gx", "gz", "gy")),
        check_vma=False,
    )
```

```python
import functools

import jax
import jax.numpy as jnp
from jax import lax
from jax.experimental import pallas as pl
from jax.experimental.pallas import tpu as pltpu
from jax.sharding import PartitionSpec as P

PROBES = 8
LEVELS = 256
LANES = 128
SITES = 4
STRIP = 12
PAD = 4
GROUP = 2

disorder_width = 4.0
spectral_scale = 8.4
MESH = pl.DeviceIdType.MESH


def kernel(names, sizes, p_hbm, d_hbm, prow_hbm, drow_hbm, mom_ref, prev_ref, cur_ref,
           p_ref, d_ref, words, packs, strips, v0, v1, v2, en, s0, s1, se, g0, g1, g2, moms, ruler,
           load_sem, send_sem, recv_sem, msend_sem, mrecv_sem, above, entered):
    X, W, _ = p_ref.shape
    Z = SITES * W
    nbx = packs.shape[0]
    M = nbx * X
    gx, gy, gz = sizes["gx"], sizes["gy"], sizes["gz"]
    ix, iy, iz = (lax.axis_index(a) for a in ("gx", "gy", "gz"))
    total = gx * gy * gz
    me = (ix * gy + iy) * gz + iz
    last = gz - 1
    staged = gx <= 3 and gy <= 4 and 3 <= gz <= 4

    def device(x, y, z):
        at = {"gx": x, "gy": y, "gz": z}
        return tuple(at[a] for a in names)

    loads = [pltpu.make_async_copy(src, dst, load_sem.at[n]) for n, (src, dst) in enumerate((
        (p_hbm, p_ref), (d_hbm, d_ref),
        (prow_hbm, words.at[0, pl.ds(0, X), pl.ds(1, W)]), (drow_hbm, words.at[1, pl.ds(0, X), pl.ds(1, W)])))]
    for load in loads:
        load.start()

    def around(at, size):
        steps = [at]
        for _ in range(size - 1):
            steps.append(jnp.where(steps[-1] + 1 == size, 0, steps[-1] + 1))
        return steps

    around_x, around_y = around(ix, gx), around(iy, gy)

    def plane_of_others(z, act):
        for x in range(gx):
            for y in range(gy):
                if x or y:
                    act(device(around_x[x], around_y[y], z))

    def each_other(act):
        def step(z, _):
            @pl.when(z != iz)
            def _():
                act(device(ix, iy, z))
            plane_of_others(z, act)
            return 0
        lax.fori_loop(0, gz, step, 0)

    xs = (0, 1) if nbx == 2 else (0, 1, -1)
    ys = (0, 1, -1)

    def at_offset(ox, oy, oz):
        return device(lax.rem(ix + ox + gx, gx), lax.rem(iy + oy + gy, gy), lax.rem(iz + oz + gz, gz))

    barrier = pltpu.get_barrier_semaphore()

    def tell(semaphore, to):
        pl.semaphore_signal(semaphore, inc=1, device_id=to, device_id_type=MESH)

    def greet(to):
        tell(barrier, to)

    per_plane = len(xs) * len(ys)
    if staged:
        plane_of_others(last, greet)

        @pl.when(iz < last)
        def _():
            greet(device(ix, iy, last))
            for ox in xs:
                for oy in ys:
                    if ox or oy:
                        greet(at_offset(ox, oy, 0))

        @pl.when(iz + 1 < last)
        def _():
            for ox in xs:
                for oy in ys:
                    greet(at_offset(ox, oy, 1))
    else:
        each_other(greet)

    lane = lax.broadcasted_iota(jnp.int32, (2 * X, LANES), 1)
    slot_word = (lane * 10923) >> 17
    column = lane - STRIP * slot_word

    for load in loads:
        load.wait()
    pack = jnp.zeros((2 * X, LANES), jnp.int32)
    for w in range(W):
        rows = jnp.concatenate([p_ref[:, w, :], d_ref[:, w, :]], axis=0)
        base = STRIP * (w + 1)
        first = pltpu.roll(rows, (base - (LANES - 3)) % LANES, 1)
        second = pltpu.roll(rows, (base + 5 - (LANES - 2)) % LANES, 1)
        pack = jnp.where(slot_word == w + 1, jnp.where(column < 5, first, second), pack)
    packs[0, 1, 1] = pack

    if staged:
        @pl.when(iz == last)
        def _():
            pl.semaphore_wait(barrier, total - 1)

        @pl.when(iz == 0)
        def _():
            pl.semaphore_wait(barrier, per_plane - 1)

        @pl.when((iz > 0) & (iz < last))
        def _():
            pl.semaphore_wait(barrier, 2 * per_plane - 1)
    else:
        pl.semaphore_wait(barrier, total - 1)

    slot_of = {0: 0, 1: nbx - 1, -1: 1}
    groups, lengths = [[] for _ in range(4)], [0] * 4
    near, far, rise, fall = range(4)
    for oz in (0, 1, -1):
        for ox in xs:
            for oy in ys:
                if ox == 0 and oz == 0 and oy == 0:
                    continue
                s = slot_of[ox]
                moves = []
                if oy == 0:
                    src_w, dst_w = {0: (pl.ds(1, W), pl.ds(1, W)), 1: (pl.ds(W, 1), pl.ds(0, 1)),
                                    -1: (pl.ds(1, 1), pl.ds(W + 1, 1))}[oz]
                    for f in range(2):
                        moves.append((words.at[f, pl.ds(0, X), src_w], words.at[f, pl.ds(s * X, X), dst_w],
                                      X * (W if oz == 0 else 1)))
                moves.append((packs.at[0, 1, 1], packs.at[s, 1 - oz, 1 - oy], 2 * X))
                g = {1: rise, -1: fall, 0: far if ox else near}[oz]
                for src, dst, length in moves:
                    lengths[g] += length
                    groups[g].append(pltpu.make_async_remote_copy(
                        src_ref=src, dst_ref=dst, send_sem=send_sem.at[g], recv_sem=recv_sem.at[g],
                        device_id=at_offset(ox, oy, oz), device_id_type=MESH))

    def start(g):
        for copy in groups[g]:
            copy.start()

    def arrive(sem, g):
        span = ruler.at[pl.ds(0, lengths[g])]
        pltpu.make_async_copy(span, span, sem).wait()

    if staged:
        @pl.when(iz == last)
        def _():
            start(rise)

        start(far)
        start(near)

        @pl.when(iz > 0)
        def _():
            start(fall)
            for ox in xs:
                for oy in ys:
                    tell(above, at_offset(ox, oy, -1))

        @pl.when(iz == last)
        def _():
            for z in range(last):
                tell(entered, device(ix, iy, z))
    else:
        for g in (rise, far, near, fall):
            start(g)

    e_mul = disorder_width / LEVELS
    e_add = disorder_width * (0.5 / LEVELS - 0.5)
    two_mul = 2.0 / (spectral_scale * spectral_scale)
    three_mul = 2.0 / spectral_scale
    one_mul = 1.0 / spectral_scale
    probe = lax.broadcasted_iota(jnp.int32, (PROBES, LANES), 0)
    lane8 = lax.broadcasted_iota(jnp.int32, (PROBES, LANES), 1)
    col8 = lane8 - STRIP * ((lane8 * 10923) >> 17)
    lifts = [31 - (SITES * probe + j) for j in range(SITES)]
    zero = jnp.zeros((PROBES, LANES), jnp.float32)

    def sign_of(row, j):
        return jnp.where((jnp.broadcast_to(row, (PROBES, LANES)) << lifts[j]) < 0, 1.0, -1.0).astype(jnp.float32)

    def energy_of(row, j):
        level = (jnp.broadcast_to(row, (PROBES, LANES)) >> (8 * j)) & 255
        return level.astype(jnp.float32) * e_mul + e_add

    def plane(e):
        return lax.rem(e + M, M)

    def around_plane(e):
        return plane(e), plane(e + 1), plane(e + M - 1)

    def loop(low, high, body):
        def step(i, _):
            body(i)
            return 0
        lax.fori_loop(low, high, step, 0)

    def edge_of(tile):
        return jnp.where(col8 == 1, pltpu.roll(tile, LANES - 6, 1), tile)

    def strip_sum(src, q, up, down):
        mine = [src[q, j] for j in range(SITES)]
        sums = []
        for j in range(SITES):
            z_up = mine[j + 1] if j + 1 < SITES else pltpu.roll(mine[0], LANES - STRIP, 1)
            z_down = mine[j - 1] if j > 0 else pltpu.roll(mine[SITES - 1], STRIP, 1)
            sums.append(src[up, j] + src[down, j] + pltpu.roll(mine[j], LANES - 1, 1)
                        + pltpu.roll(mine[j], 1, 1) + z_up + z_down)
        return mine, sums

    def rows_of(src, edges, q, up, down, w):
        fields = [src[q, SITES * w + r] for r in range(SITES * GROUP + 2)]
        for r in range(SITES * GROUP):
            row = SITES * w + r + 1
            turn = lax.rem(2 * LANES - 2 - STRIP * (w + r // SITES), LANES)
            fix = pltpu.roll(edges[q, r % SITES], turn, 1)
            mid = fields[r + 1]
            right = jnp.where(lane8 == LANES - 1, fix, pltpu.roll(mid, LANES - 1, 1))
            left = jnp.where(lane8 == 0, fix, pltpu.roll(mid, 1, 1))
            yield row, mid, src[up, row] + src[down, row] + right + left + fields[r + 2] + fields[r]

    def level_one(q, up, down, w):
        for row, mid, six in rows_of(v0, g0, q, up, down, w):
            v1[q, row] = en[q, row] * mid - six

    def level_two(q, up, down, w, first, final, sums):
        a, b, c = sums
        for row, mid, six in rows_of(v1, g1, q, up, down, w):
            begin = v0[q, row]
            new = two_mul * (en[q, row] * mid - six) - begin
            v2[q, row] = new
            counts = (row >= first) & (row <= final)
            part = jnp.where(counts, mid, 0.0)
            a, b, c = a + begin * part, b + part * part, c + part * jnp.where(counts, new, 0.0)
        return a, b, c

    def level_three(q, up, down, w):
        for n, (row, mid, six) in enumerate(rows_of(v2, g2, q, up, down, w)):
            at = pl.ds(q * Z + SITES * (w - 1) + n, PROBES, stride=X * Z + PAD)
            prev_ref[at, :] = mid
            cur_ref[at, :] = three_mul * (en[q, row] * mid - six) - one_mul * v1[q, row]

    def strip_one(e):
        q, up, down = around_plane(e)
        mine, six = strip_sum(s0, q, up, down)
        for j in range(SITES):
            new = se[q, j] * mine[j] - six[j]
            s1[q, j] = new
            g1[q, j] = edge_of(new)

    def strip_two(x):
        q, up, down = around_plane(x)
        mine, six = strip_sum(s1, q, up, down)
        for j in range(SITES):
            g2[q, j] = edge_of(two_mul * (se[q, j] * mine[j] - six[j]) - s0[q, j])

    def unpack_word(q, w):
        for j in range(SITES):
            row = SITES * w + j + 1
            v0[q, row] = sign_of(words[0, q, w], j)
            en[q, row] = energy_of(words[1, q, w], j)

    def unpack_strip(s, x):
        q = s * X + x
        for j in range(SITES):
            sign = sign_of(strips[s, pl.ds(x, 1)], j)
            s0[q, j] = sign
            g0[q, j] = edge_of(sign)
            se[q, j] = energy_of(strips[s, pl.ds(X + x, 1)], j)

    def send_moments(sums):
        row = zero
        for n, acc in enumerate(sums):
            summed = jnp.broadcast_to(jnp.sum(acc, axis=1, keepdims=True), (PROBES, LANES))
            row = row + jnp.where(lane8 == PROBES * n + probe, summed, 0.0)
        moms[me] = jnp.sum(row, axis=0, keepdims=True)
        each_other(lambda to: pltpu.make_async_remote_copy(
            src_ref=moms.at[me], dst_ref=moms.at[me], send_sem=msend_sem, recv_sem=mrecv_sem,
            device_id=to, device_id_type=MESH).start())

    def pick(n, values):
        chosen = values[-1]
        for m in range(len(values) - 1):
            chosen = jnp.where(n == m, values[m], chosen)
        return chosen

    def stage(n, sums):
        up = (n == 2) != (iz == last)
        inner = (n < 2) | (n == 4)

        @pl.when(n == 0)
        def _():
            arrive(recv_sem.at[near], near)

        @pl.when(n == 1)
        def _():
            arrive(recv_sem.at[far], far)
            if staged:
                @pl.when(iz < last)
                def _():
                    pl.semaphore_wait(above, per_plane)
                    start(rise)

        @pl.when(jnp.logical_not(inner) & up)
        def _():
            arrive(recv_sem.at[fall], fall)

        @pl.when(jnp.logical_not(inner) & jnp.logical_not(up))
        def _():
            arrive(recv_sem.at[rise], rise)

        side_word = jnp.where(up, W + 1, 0)
        slot_low = pick(n, (0, 1, 0, 0, nbx))
        slot_high = pick(n, (1, nbx))
        word_low = jnp.where(inner, 1, side_word)
        word_high = jnp.where(inner, W + 1, side_word + 1)
        which = jnp.where(inner, 1, jnp.where(up, 2, 0))
        turn = jnp.where(inner, 0, jnp.where(up, STRIP * W % LANES, (LANES - STRIP * W % LANES) % LANES))

        def unpack_slot(s):
            joined = jnp.where(column < 3, packs[s, which, 0], jnp.where(column < 7, packs[s, which, 1], packs[s, which, 2]))
            taken = jnp.broadcast_to(inner, slot_word.shape) | (slot_word == side_word)
            strips[s] = jnp.where(taken, pltpu.roll(joined, turn, 1), strips[s])

            def unpack_plane(x):
                unpack_strip(s, x)
                loop(word_low, word_high, lambda w: unpack_word(s * X + x, w))
            loop(0, X, unpack_plane)

        loop(slot_low, slot_high, unpack_slot)

        group_low = jnp.where(inner, 1, jnp.where(up, W + 1 - GROUP + 1, 0))
        groups_here = jnp.where(inner, W // GROUP, 1)

        def one(i):
            e = pick(n, (1, -1, -1, -1, -2)) + i + jnp.where(i >= pick(n, (X, 2, M, M, 1)), pick(n, (0, X - 2, 0, 0, X + 2)), 0)
            strip_one(e)
            at = around_plane(e)
            loop(0, groups_here, lambda g: level_one(*at, group_low + GROUP * g))

        loop(0, pick(n, (X - 2, 4, X + 2, X + 2, 2)), one)
        weigh = pick(n, (False, True, (iz != last) & up | (iz == 0) & jnp.logical_not(up), (iz != last) & up | (iz == 0) & jnp.logical_not(up), False))
        row_low = jnp.where(inner, 2, jnp.where(up, Z - 2, -2))
        row_high = jnp.where(weigh, jnp.where(inner, Z - 3, jnp.where(up, Z + 1, 1)), -Z)

        def two(i, sums):
            e = jnp.where(n == 4, (X + 1) * i - 1, i)
            at = around_plane(e)
            return lax.fori_loop(0, groups_here, lambda g, sums: level_two(
                *at, group_low + GROUP * g, row_low + SITES + 1, row_high + SITES + 1, sums), sums)

        sums = lax.fori_loop(0, pick(n, (0, X, X, X, 2)), two, sums)

        @pl.when(n == jnp.where(iz == last, 1, jnp.where(iz == 0, 3, 2)))
        def _():
            if staged:
                @pl.when((iz > 0) & (iz < last))
                def _():
                    pl.semaphore_wait(entered, 1)
            send_moments(sums)

        if staged:
            @pl.when((n == 2) & (iz == 0))
            def _():
                pl.semaphore_wait(entered, 1)
                start(fall)
        return sums

    lax.fori_loop(0, 5, stage, (zero, zero, zero))
    loop(0, X, strip_two)

    def three(x):
        at = around_plane(x)
        loop(0, W // GROUP, lambda g: level_three(*at, 1 + GROUP * g))

    loop(0, X, three)

    others = moms.at[pl.ds(0, total - 1)]
    pltpu.make_async_copy(others, others, mrecv_sem).wait()
    sites = total * X * Z * LANES
    sums = jnp.sum(moms[...], axis=0) * (1.0 / sites)
    first = one_mul * sums
    second = two_mul * pltpu.roll(sums, LANES - PROBES, 1) - 1.0
    third = three_mul * pltpu.roll(sums, LANES - 2 * PROBES, 1) - first
    mom_ref[...] = jnp.concatenate([first, second, third], axis=0)[:, :PROBES]
    pltpu.make_async_copy(others, others, msend_sem).wait()
    for g in range(4):
        arrive(send_sem.at[g], g)


def write_out(mom_ref, prev_ref, cur_ref, mom_hbm, prev_hbm, cur_hbm, sem):
    rows = prev_hbm.shape[0] // PROBES
    copies = [pltpu.make_async_copy(mom_ref, mom_hbm, sem.at[2 * PROBES])]
    for n, (src, dst) in enumerate(((prev_ref, prev_hbm), (cur_ref, cur_hbm))):
        for r in range(PROBES):
            copies.append(pltpu.make_async_copy(
                src.at[pl.ds(r * (rows + PAD), rows)], dst.at[pl.ds(r * rows, rows)], sem.at[n * PROBES + r]))
    for copy in copies:
        copy.start()
    for copy in copies:
        copy.wait()


def per_device(names, sizes, probe_bits, disorder_levels):
    X, W, Y = probe_bits.shape
    if Y != LANES or STRIP * (W + 2) > LANES or X < 3 or W % GROUP:
        raise ValueError("block size")
    Z = SITES * W
    nbx = 2 if sizes["gx"] == 2 else 3
    M = nbx * X
    total = sizes["gx"] * sizes["gy"] * sizes["gz"]
    rows = (X, W, 1, Y)
    vmem = pl.BlockSpec(memory_space=pltpu.VMEM)
    f32, i32 = jnp.float32, jnp.int32
    tile = (PROBES, LANES)
    hbm = pl.BlockSpec(memory_space=pltpu.HBM)
    out_shape = (
        jax.ShapeDtypeStruct((3, PROBES), f32),
        jax.ShapeDtypeStruct((PROBES * X * Z, Y), f32),
        jax.ShapeDtypeStruct((PROBES * X * Z, Y), f32),
    )
    padded = jax.ShapeDtypeStruct((PROBES * (X * Z + PAD), Y), f32)
    padded_shape = (out_shape[0], padded, padded)
    results = pl.pallas_call(
        functools.partial(kernel, names, sizes),
        out_shape=padded_shape,
        in_specs=[hbm] * 4,
        out_specs=(vmem,) * 3,
        scratch_shapes=[
            pltpu.VMEM((X, W, Y), i32),
            pltpu.VMEM((X, W, Y), i32),
            pltpu.VMEM((2, M, W + 2, 1, LANES), i32),
            pltpu.VMEM((nbx, 3, 3, 2 * X, LANES), i32),
            pltpu.VMEM((nbx, 2 * X, LANES), i32),
            pltpu.VMEM((M, Z + 2 * SITES + 2) + tile, f32),
            pltpu.VMEM((M, Z + 2 * SITES + 2) + tile, f32),
            pltpu.VMEM((M, Z + 2 * SITES + 2) + tile, f32),
            pltpu.VMEM((M, Z + 2 * SITES + 2) + tile, f32),
            pltpu.VMEM((M, SITES) + tile, f32),
            pltpu.VMEM((M, SITES) + tile, f32),
            pltpu.VMEM((M, SITES) + tile, f32),
            pltpu.VMEM((M, SITES) + tile, f32),
            pltpu.VMEM((M, SITES) + tile, f32),
            pltpu.VMEM((M, SITES) + tile, f32),
            pltpu.VMEM((total, 1, LANES), f32),
            pltpu.VMEM((X * (2 * W + 6) * nbx, LANES), i32),
            pltpu.SemaphoreType.DMA((4,)),
            pltpu.SemaphoreType.DMA((4,)),
            pltpu.SemaphoreType.DMA((4,)),
            pltpu.SemaphoreType.DMA,
            pltpu.SemaphoreType.DMA,
            pltpu.SemaphoreType.REGULAR,
            pltpu.SemaphoreType.REGULAR,
        ],
        compiler_params=pltpu.CompilerParams(collective_id=0, has_side_effects=True,
                                             vmem_limit_bytes=40 * 1024 * 1024),
    )(*[pltpu.with_memory_space_constraint(a, pltpu.HBM) for a in (probe_bits, disorder_levels, probe_bits.reshape(rows), disorder_levels.reshape(rows))])
    moments, previous, current = pl.pallas_call(
        write_out,
        out_shape=out_shape,
        in_specs=[vmem] * 3,
        out_specs=(hbm,) * 3,
        scratch_shapes=[pltpu.SemaphoreType.DMA((2 * PROBES + 1,))],
        compiler_params=pltpu.CompilerParams(vmem_limit_bytes=16 * 1024 * 1024),
    )(*results)
    shape = (PROBES, X, Z, Y)
    return moments, previous.reshape(shape), current.reshape(shape)


def solution(mesh):
    placed = (P("gx", "gz", "gy"), P("gx", "gz", "gy"))
    sizes = {a: mesh.shape[a] for a in mesh.axis_names}
    return jax.shard_map(
        functools.partial(per_device, tuple(mesh.axis_names), sizes),
        mesh=mesh,
        in_specs=placed,
        out_specs=(P(), P(None, "gx", "gz", "gy"), P(None, "gx", "gz", "gy")),
        check_vma=False,
    )
```

```python
import functools

import jax
import jax.numpy as jnp
from jax import lax
from jax.experimental import pallas as pl
from jax.experimental.pallas import tpu as pltpu
from jax.sharding import PartitionSpec as P

PROBES = 8
LEVELS = 256
LANES = 128
SITES = 4
STRIP = 12
PAD = 4

disorder_width = 4.0
spectral_scale = 8.4
MESH = pl.DeviceIdType.MESH


def kernel(names, sizes, p_hbm, d_hbm, prow_hbm, drow_hbm, mom_ref, prev_ref, cur_ref,
           p_ref, d_ref, words, lefts, rights, packs, strips, v0, v1, v2, en, s0, s1, se, g1, g2, turned, accs, moms,
           load_sem, send_sem, recv_sem, msend_sem, mrecv_sem, above, entered):
    X, W, _ = p_ref.shape
    Z = SITES * W
    nbx = packs.shape[0]
    M = nbx * X
    gx, gy, gz = sizes["gx"], sizes["gy"], sizes["gz"]
    ix, iy, iz = (lax.axis_index(a) for a in ("gx", "gy", "gz"))
    total = gx * gy * gz
    me = (ix * gy + iy) * gz + iz
    last = gz - 1
    staged = gx <= 3 and gy <= 4 and 3 <= gz <= 4

    def device(x, y, z):
        at = {"gx": x, "gy": y, "gz": z}
        return tuple(at[a] for a in names)

    loads = [pltpu.make_async_copy(src, dst, load_sem.at[n]) for n, (src, dst) in enumerate((
        (p_hbm, p_ref), (d_hbm, d_ref),
        (prow_hbm, words.at[0, pl.ds(0, X), pl.ds(1, W)]), (drow_hbm, words.at[1, pl.ds(0, X), pl.ds(1, W)])))]
    for load in loads:
        load.start()

    def around(at, size):
        steps = [at]
        for _ in range(size - 1):
            steps.append(jnp.where(steps[-1] + 1 == size, 0, steps[-1] + 1))
        return steps

    around_x, around_y = around(ix, gx), around(iy, gy)

    def plane_of_others(z, act):
        for x in range(gx):
            for y in range(gy):
                if x or y:
                    act(device(around_x[x], around_y[y], z))

    def whole_plane(z, act):
        for x in range(gx):
            for y in range(gy):
                act(device(around_x[x], around_y[y], z))

    def each_other(act):
        if gz <= 4:
            for z in range(gz):
                @pl.when(iz != z)
                def _(z=z):
                    whole_plane(z, act)
        else:
            def step(n, _):
                whole_plane(lax.rem(iz + n, gz), act)
                return 0
            lax.fori_loop(1, gz, step, 0)
        plane_of_others(iz, act)

    xs = (0, 1) if nbx == 2 else (0, 1, -1)
    ys = (0, 1, -1)

    def at_offset(ox, oy, oz):
        return device(lax.rem(ix + ox + gx, gx), lax.rem(iy + oy + gy, gy), lax.rem(iz + oz + gz, gz))

    barrier = pltpu.get_barrier_semaphore()

    def greet(to):
        pl.semaphore_signal(barrier, inc=1, device_id=to, device_id_type=MESH)

    per_plane = len(xs) * len(ys)
    if staged:
        @pl.when(iz < last)
        def _():
            whole_plane(last, greet)
            for ox in xs:
                for oy in ys:
                    if ox or oy:
                        greet(at_offset(ox, oy, 0))

        @pl.when(iz == last)
        def _():
            plane_of_others(iz, greet)

        @pl.when(iz + 1 < last)
        def _():
            for ox in xs:
                for oy in ys:
                    greet(at_offset(ox, oy, 1))
    else:
        each_other(greet)

    lane = lax.broadcasted_iota(jnp.int32, (2 * X, LANES), 1)
    slot_word = (lane * 10923) >> 17
    column = lane - STRIP * slot_word

    for load in loads:
        load.wait()
    pack = jnp.zeros((2 * X, LANES), jnp.int32)
    for w in range(W):
        rows = jnp.concatenate([p_ref[:, w, :], d_ref[:, w, :]], axis=0)
        base = STRIP * (w + 1)
        first = pltpu.roll(rows, (base - (LANES - 3)) % LANES, 1)
        second = pltpu.roll(rows, (base + 5 - (LANES - 2)) % LANES, 1)
        pack = jnp.where(slot_word == w + 1, jnp.where(column < 5, first, second), pack)
    packs[0, 1, 1] = pack

    if staged:
        @pl.when(iz == last)
        def _():
            pl.semaphore_wait(barrier, total - 1)

        @pl.when(iz == 0)
        def _():
            pl.semaphore_wait(barrier, per_plane - 1)

        @pl.when((iz > 0) & (iz < last))
        def _():
            pl.semaphore_wait(barrier, 2 * per_plane - 1)
    else:
        pl.semaphore_wait(barrier, total - 1)

    slot_of = {0: 0, 1: nbx - 1, -1: 1}
    groups = {"far": [], "near": [], 1: [], -1: []}
    count = 0
    for oz in (0, 1, -1):
        for ox in xs:
            for oy in ys:
                if ox == 0 and oz == 0 and oy == 0:
                    continue
                s = slot_of[ox]
                moves = []
                if oy == 0:
                    src_w, dst_w = {0: (pl.ds(1, W), pl.ds(1, W)), 1: (pl.ds(W, 1), pl.ds(0, 1)),
                                    -1: (pl.ds(1, 1), pl.ds(W + 1, 1))}[oz]
                    for f in range(2):
                        moves.append((words.at[f, pl.ds(0, X), src_w], words.at[f, pl.ds(s * X, X), dst_w]))
                moves.append((packs.at[0, 1, 1], packs.at[s, 1 - oz, 1 - oy]))
                for src, dst in moves:
                    groups[oz if oz else ("far" if ox else "near")].append(pltpu.make_async_remote_copy(
                        src_ref=src, dst_ref=dst, send_sem=send_sem.at[count], recv_sem=recv_sem.at[count],
                        device_id=at_offset(ox, oy, oz), device_id_type=MESH))
                    count += 1

    def start(copies):
        for copy in copies:
            copy.start()

    def tell(semaphore, to):
        pl.semaphore_signal(semaphore, inc=1, device_id=to, device_id_type=MESH)

    if staged:
        @pl.when(iz == last)
        def _():
            start(groups[1])

        start(groups["far"] + groups["near"])

        @pl.when(iz > 0)
        def _():
            start(groups[-1])
            for ox in xs:
                for oy in ys:
                    tell(above, at_offset(ox, oy, -1))

        @pl.when(iz == last)
        def _():
            for z in range(last):
                tell(entered, device(ix, iy, z))
    else:
        start(groups[1] + groups["far"] + groups["near"] + groups[-1])

    e_mul = disorder_width / LEVELS
    e_add = disorder_width * (0.5 / LEVELS - 0.5)
    two_mul = 2.0 / (spectral_scale * spectral_scale)
    three_mul = 2.0 / spectral_scale
    one_mul = 1.0 / spectral_scale
    probe = lax.broadcasted_iota(jnp.int32, (PROBES, LANES), 0)
    lane8 = lax.broadcasted_iota(jnp.int32, (PROBES, LANES), 1)
    slot8 = (lane8 * 10923) >> 17
    col8 = lane8 - STRIP * slot8
    lifts = [31 - (SITES * probe + j) for j in range(SITES)]
    zero = jnp.zeros((PROBES, LANES), jnp.float32)

    def sign_of(row, j):
        return jnp.where((jnp.broadcast_to(row, (PROBES, LANES)) << lifts[j]) < 0, 1.0, -1.0).astype(jnp.float32)

    def energy_of(row, j):
        level = (jnp.broadcast_to(row, (PROBES, LANES)) >> (8 * j)) & 255
        return level.astype(jnp.float32) * e_mul + e_add

    def unpack(q, zs):
        for z in zs:
            w, j = divmod(z + SITES, SITES)
            v0[q, z + SITES] = sign_of(words[0, q, w], j)
            en[q, z + SITES] = energy_of(words[1, q, w], j)

    def plane(e):
        return lax.rem(e + M, M)

    def planes(low, high, body):
        def step(i, _):
            body(plane(i - low))
            return 0
        lax.fori_loop(0, min(M, X + low + high), step, 0)

    def join_strips(s, oz):
        return jnp.where(column < 3, packs[s, oz, 0], jnp.where(column < 7, packs[s, oz, 1], packs[s, oz, 2]))

    def shift_words(s, ws):
        own = pl.ds(s * X, X)
        edges = jnp.where(column == 1, pltpu.roll(strips[s], LANES - 6, 1), strips[s])[:X]
        for w in ws:
            rows = words[0, own, w, 0, :]
            fix = pltpu.roll(edges, (-(STRIP * w + 2)) % LANES, 1)
            rights[own, w, 0, :] = jnp.where(lane[:X] == LANES - 1, fix, pltpu.roll(rows, LANES - 1, 1))
            lefts[own, w, 0, :] = jnp.where(lane[:X] == 0, fix, pltpu.roll(rows, 1, 1))

    def unpack_strips(s):
        for n, turn in enumerate((LANES - 1, 1, LANES - STRIP, STRIP)):
            turned[s, n] = pltpu.roll(strips[s], turn, 1)
        for x in range(X):
            for j in range(SITES):
                s0[s * X + x, j] = sign_of(strips[s, x:x + 1], j)
                se[s * X + x, j] = energy_of(strips[s, X + x:X + x + 1], j)

    def strip_one(q):
        s, x = divmod(q, X)
        for j in range(SITES):
            right, left, z_up, z_down = (turned[s, n, x:x + 1] for n in range(4))
            mine = s0[q, j]
            six = (s0[(q + 1) % M, j] + s0[(q + M - 1) % M, j] + sign_of(right, j) + sign_of(left, j)
                   + (s0[q, j + 1] if j + 1 < SITES else sign_of(z_up, 0))
                   + (s0[q, j - 1] if j > 0 else sign_of(z_down, SITES - 1)))
            new = se[q, j] * mine - six
            s1[q, j] = new
            g1[q, j] = edge_of(new)

    def strips_one():
        for q in sorted({e % M for e in range(-1, X + 1)}):
            strip_one(q)

    def strip_sum(src, q, up, down):
        mine = [src[q, j] for j in range(SITES)]
        sums, rights, ups = [], [], []
        for j in range(SITES):
            z_up = mine[j + 1] if j + 1 < SITES else pltpu.roll(mine[0], LANES - STRIP, 1)
            z_down = mine[j - 1] if j > 0 else pltpu.roll(mine[SITES - 1], STRIP, 1)
            sums.append(src[up, j] + src[down, j] + pltpu.roll(mine[j], LANES - 1, 1)
                        + pltpu.roll(mine[j], 1, 1) + z_up + z_down)
        return mine, sums

    def edge_of(tile):
        return jnp.where(col8 == 1, pltpu.roll(tile, LANES - 6, 1), tile)

    def site_sum(src, q, up, down, z, edges):
        w, j = divmod(z + SITES, SITES)
        fix = pltpu.roll(edges[q, j], (-(STRIP * w + 2)) % LANES, 1)
        mid = src[q, z + SITES]
        right = jnp.where(lane8 == LANES - 1, fix, pltpu.roll(mid, LANES - 1, 1))
        left = jnp.where(lane8 == 0, fix, pltpu.roll(mid, 1, 1))
        return mid, src[up, z + SITES] + src[down, z + SITES] + right + left + src[q, z + SITES + 1] + src[q, z + SITES - 1]

    def around_plane(e):
        return plane(e), plane(e + 1), plane(e + M - 1)

    def level_one(e, zs):
        q, up, down = around_plane(e)
        for z in zs:
            w, j = divmod(z + SITES, SITES)
            at = z + SITES
            total_six = (v0[up, at] + v0[down, at] + sign_of(rights[q, w], j) + sign_of(lefts[q, w], j)
                         + v0[q, at + 1] + v0[q, at - 1])
            v1[q, at] = en[q, at] * v0[q, at] - total_six

    def level_two(e, zs, sums):
        q, up, down = around_plane(e)
        for z in zs:
            mid, total_six = site_sum(v1, q, up, down, z, g1)
            start = v0[q, z + SITES]
            new = two_mul * (en[q, z + SITES] * mid - total_six) - start
            v2[q, z + SITES] = new
            if sums is not None:
                sums = sums[0] + start * mid, sums[1] + mid * mid, sums[2] + mid * new
        return sums

    def strips_two():
        for q in range(X):
            mine, six = strip_sum(s1, q, q + 1, (q + M - 1) % M)
            for j in range(SITES):
                g2[q, j] = edge_of(two_mul * (se[q, j] * mine[j] - six[j]) - s0[q, j])

    def level_three(x, zs):
        q, up, down = around_plane(x)
        for z in zs:
            mid, total_six = site_sum(v2, q, up, down, z, g2)
            new = three_mul * (en[q, z + SITES] * mid - total_six) - one_mul * v1[q, z + SITES]
            at = pl.ds(x * Z + z, PROBES, stride=X * Z + PAD)
            prev_ref[at, :] = mid
            cur_ref[at, :] = new

    def loop(low, high, body):
        def step(i, _):
            body(i)
            return 0
        lax.fori_loop(low, high, step, 0)

    def own_two(zs):
        return lax.fori_loop(0, X, lambda x, sums: level_two(x, zs, sums), (zero, zero, zero))

    def send_moments(sums):
        row = zero
        for n, acc in enumerate(sums):
            summed = jnp.broadcast_to(jnp.sum(acc, axis=1, keepdims=True), (PROBES, LANES))
            row = row + jnp.where(lane8 == PROBES * n + probe, summed, 0.0)
        moms[me] = jnp.sum(row, axis=0, keepdims=True)
        each_other(lambda to: pltpu.make_async_remote_copy(
            src_ref=moms.at[me], dst_ref=moms.at[me], send_sem=msend_sem, recv_sem=mrecv_sem,
            device_id=to, device_id_type=MESH).start())

    def unpack_own(x, _):
        unpack(x, range(Z))
        return 0

    def unpack_far(i, _):
        unpack(plane(X + i), range(Z))
        return 0

    def unpack_low(i, _):
        unpack(plane(i - 3), range(Z))
        return 0

    lax.fori_loop(0, X, unpack_own, 0)
    for copy in groups["near"]:
        copy.wait_recv()
    strips[0] = join_strips(0, 1)
    shift_words(0, range(1, W + 1))
    unpack_strips(0)
    main = range(1, Z - 1)
    loop(1, X - 1, lambda x: level_one(x, main))
    for copy in groups["far"]:
        copy.wait_recv()
    for s in range(1, nbx):
        strips[s] = join_strips(s, 1)
        shift_words(s, range(1, W + 1))
        unpack_strips(s)
    if M <= X + 6:
        lax.fori_loop(0, M - X, unpack_far, 0)
    else:
        lax.fori_loop(0, 3, unpack_far, 0)
        lax.fori_loop(0, 3, unpack_low, 0)

    if staged:
        @pl.when(iz < last)
        def _():
            pl.semaphore_wait(above, per_plane)
            start(groups[1])

    def ends_of(low):
        width = X - 1 - 2 * low

        def body(i):
            level_one(low + i * width, main)
        return body

    strips_one()
    loop(0, 2, ends_of(0))
    loop(0, 2, ends_of(-1))
    sums = own_two(range(2, Z - 2))
    for n in range(3):
        accs[n] = sums[n]

    @pl.when(iz == last)
    def _():
        send_moments([accs[n] for n in range(3)])

    loop(0, min(M, X + 4) - (X + 2), ends_of(-2))

    def side(up):
        for copy in groups[-1 if up else 1]:
            copy.wait_recv()
        outside = range(Z, Z + SITES) if up else range(-SITES, 0)
        planes(3, 3, lambda q: unpack(q, outside))
        for s in range(nbx):
            if up:
                strips[s] = jnp.where(slot_word == W + 1, pltpu.roll(join_strips(s, 2), (STRIP * W) % LANES, 1), strips[s])
            else:
                strips[s] = jnp.where(slot_word == 0, pltpu.roll(join_strips(s, 0), (-STRIP * W) % LANES, 1), strips[s])
            shift_words(s, [W + 1 if up else 0])
            unpack_strips(s)
        ones = range(Z - 1, Z + 3) if up else range(-3, 1)
        twos = range(Z - 2, Z + 2) if up else range(-2, 2)
        strips_one()
        loop(0, min(M, X + 4), lambda i: level_one(i - 2, ones))
        sums = (zero, zero, zero)
        for x in range(X):
            sums = level_two(x, twos, sums)
        on = (iz != last) if up else (iz == 0)
        for n in range(3):
            accs[n] = accs[n] + jnp.where(on, sums[n], 0.0)

        if up:
            @pl.when((iz > 0) & (iz < last))
            def _():
                if staged:
                    pl.semaphore_wait(entered, 1)
                send_moments([accs[n] for n in range(3)])
        else:
            @pl.when(iz == 0)
            def _():
                send_moments([accs[n] for n in range(3)])

    def finish(zs):
        loop(0, 2, lambda i: level_two(i * (X + 1) - 1, zs, None))
        strips_two()
        loop(0, X, lambda x: level_three(x, zs))

    @pl.when(iz == last)
    def _():
        side(False)
        finish(range(Z - 3))

    if staged:
        @pl.when(iz == 0)
        def _():
            pl.semaphore_wait(entered, 1)
            start(groups[-1])

    side(True)

    @pl.when(iz == last)
    def _():
        finish(range(Z - 3, Z))

    @pl.when(iz < last)
    def _():
        side(False)
        finish(range(Z))

    others = moms.at[pl.ds(0, total - 1)]
    pltpu.make_async_copy(others, others, mrecv_sem).wait()
    sites = total * X * Z * LANES
    sums = jnp.sum(moms[...], axis=0) * (1.0 / sites)
    first = one_mul * sums
    second = two_mul * pltpu.roll(sums, LANES - PROBES, 1) - 1.0
    third = three_mul * pltpu.roll(sums, LANES - 2 * PROBES, 1) - first
    mom_ref[...] = jnp.concatenate([first, second, third], axis=0)[:, :PROBES]
    pltpu.make_async_copy(others, others, msend_sem).wait()
    for group in groups.values():
        for copy in group:
            copy.wait_send()


def write_out(mom_ref, prev_ref, cur_ref, mom_hbm, prev_hbm, cur_hbm, sem):
    rows = prev_hbm.shape[0] // PROBES
    copies = [pltpu.make_async_copy(mom_ref, mom_hbm, sem.at[2 * PROBES])]
    for n, (src, dst) in enumerate(((prev_ref, prev_hbm), (cur_ref, cur_hbm))):
        for r in range(PROBES):
            copies.append(pltpu.make_async_copy(
                src.at[pl.ds(r * (rows + PAD), rows)], dst.at[pl.ds(r * rows, rows)], sem.at[n * PROBES + r]))
    for copy in copies:
        copy.start()
    for copy in copies:
        copy.wait()


def per_device(names, sizes, probe_bits, disorder_levels):
    X, W, Y = probe_bits.shape
    if Y != LANES or STRIP * (W + 2) > LANES or X < 3:
        raise ValueError("block size")
    Z = SITES * W
    nbx = 2 if sizes["gx"] == 2 else 3
    M = nbx * X
    n_copies = (9 * nbx - 1) + 2 * (3 * nbx - 1)
    total = sizes["gx"] * sizes["gy"] * sizes["gz"]
    rows = (X, W, 1, Y)
    vmem = pl.BlockSpec(memory_space=pltpu.VMEM)
    f32, i32 = jnp.float32, jnp.int32
    tile = (PROBES, LANES)
    hbm = pl.BlockSpec(memory_space=pltpu.HBM)
    out_shape = (
        jax.ShapeDtypeStruct((3, PROBES), f32),
        jax.ShapeDtypeStruct((PROBES * X * Z, Y), f32),
        jax.ShapeDtypeStruct((PROBES * X * Z, Y), f32),
    )
    padded = jax.ShapeDtypeStruct((PROBES * (X * Z + PAD), Y), f32)
    padded_shape = (out_shape[0], padded, padded)
    results = pl.pallas_call(
        functools.partial(kernel, names, sizes),
        out_shape=padded_shape,
        in_specs=[hbm] * 4,
        out_specs=(vmem,) * 3,
        scratch_shapes=[
            pltpu.VMEM((X, W, Y), i32),
            pltpu.VMEM((X, W, Y), i32),
            pltpu.VMEM((2, M, W + 2, 1, LANES), i32),
            pltpu.VMEM((M, W + 2, 1, LANES), i32),
            pltpu.VMEM((M, W + 2, 1, LANES), i32),
            pltpu.VMEM((nbx, 3, 3, 2 * X, LANES), i32),
            pltpu.VMEM((nbx, 2 * X, LANES), i32),
            pltpu.VMEM((M, Z + 2 * SITES) + tile, f32),
            pltpu.VMEM((M, Z + 2 * SITES) + tile, f32),
            pltpu.VMEM((M, Z + 2 * SITES) + tile, f32),
            pltpu.VMEM((M, Z + 2 * SITES) + tile, f32),
            pltpu.VMEM((M, SITES) + tile, f32),
            pltpu.VMEM((M, SITES) + tile, f32),
            pltpu.VMEM((M, SITES) + tile, f32),
            pltpu.VMEM((M, SITES) + tile, f32),
            pltpu.VMEM((M, SITES) + tile, f32),
            pltpu.VMEM((nbx, 4, 2 * X, LANES), i32),
            pltpu.VMEM((3,) + tile, f32),
            pltpu.VMEM((total, 1, LANES), f32),
            pltpu.SemaphoreType.DMA((4,)),
            pltpu.SemaphoreType.DMA((n_copies,)),
            pltpu.SemaphoreType.DMA((n_copies,)),
            pltpu.SemaphoreType.DMA,
            pltpu.SemaphoreType.DMA,
            pltpu.SemaphoreType.REGULAR,
            pltpu.SemaphoreType.REGULAR,
        ],
        compiler_params=pltpu.CompilerParams(collective_id=0, has_side_effects=True,
                                             vmem_limit_bytes=40 * 1024 * 1024),
    )(*[pltpu.with_memory_space_constraint(a, pltpu.HBM) for a in (probe_bits, disorder_levels, probe_bits.reshape(rows), disorder_levels.reshape(rows))])
    moments, previous, current = pl.pallas_call(
        write_out,
        out_shape=out_shape,
        in_specs=[vmem] * 3,
        out_specs=(hbm,) * 3,
        scratch_shapes=[pltpu.SemaphoreType.DMA((2 * PROBES + 1,))],
        compiler_params=pltpu.CompilerParams(vmem_limit_bytes=16 * 1024 * 1024),
    )(*results)
    shape = (PROBES, X, Z, Y)
    return moments, previous.reshape(shape), current.reshape(shape)


def solution(mesh):
    placed = (P("gx", "gz", "gy"), P("gx", "gz", "gy"))
    sizes = {a: mesh.shape[a] for a in mesh.axis_names}
    return jax.shard_map(
        functools.partial(per_device, tuple(mesh.axis_names), sizes),
        mesh=mesh,
        in_specs=placed,
        out_specs=(P(), P(None, "gx", "gz", "gy"), P(None, "gx", "gz", "gy")),
        check_vma=False,
    )
```

```python
import functools

import jax
import jax.numpy as jnp
from jax import lax
from jax.experimental import pallas as pl
from jax.experimental.pallas import tpu as pltpu
from jax.sharding import PartitionSpec as P

PROBES = 8
LEVELS = 256
LANES = 128
SITES = 4
STRIP = 12
PAD = 8

disorder_width = 4.0
spectral_scale = 8.4
MESH = pl.DeviceIdType.MESH


def kernel(names, sizes, p_hbm, d_hbm, prow_hbm, drow_hbm, mom_ref, prev_ref, cur_ref,
           p_ref, d_ref, words, lefts, rights, packs, strips, v0, v1, v2, en, s0, s1, se, g1, g2, turned, accs, moms,
           load_sem, send_sem, recv_sem, msend_sem, mrecv_sem, above, entered):
    X, W, _ = p_ref.shape
    Z = SITES * W
    nbx = packs.shape[0]
    M = nbx * X
    gx, gy, gz = sizes["gx"], sizes["gy"], sizes["gz"]
    ix, iy, iz = (lax.axis_index(a) for a in ("gx", "gy", "gz"))
    total = gx * gy * gz
    me = (ix * gy + iy) * gz + iz
    last = gz - 1
    staged = gx <= 3 and gy <= 4 and 3 <= gz <= 4

    def device(x, y, z):
        at = {"gx": x, "gy": y, "gz": z}
        return tuple(at[a] for a in names)

    loads = [pltpu.make_async_copy(src, dst, load_sem.at[n]) for n, (src, dst) in enumerate((
        (p_hbm, p_ref), (d_hbm, d_ref),
        (prow_hbm, words.at[0, pl.ds(0, X), pl.ds(1, W)]), (drow_hbm, words.at[1, pl.ds(0, X), pl.ds(1, W)])))]
    for load in loads:
        load.start()

    def around(at, size):
        steps = [at]
        for _ in range(size - 1):
            steps.append(jnp.where(steps[-1] + 1 == size, 0, steps[-1] + 1))
        return steps

    around_x, around_y = around(ix, gx), around(iy, gy)

    def plane_of_others(z, act):
        for x in range(gx):
            for y in range(gy):
                if x or y:
                    act(device(around_x[x], around_y[y], z))

    def whole_plane(z, act):
        for x in range(gx):
            for y in range(gy):
                act(device(around_x[x], around_y[y], z))

    def each_other(act):
        if gz <= 4:
            for z in range(gz):
                @pl.when(iz != z)
                def _(z=z):
                    whole_plane(z, act)
        else:
            def step(n, _):
                whole_plane(lax.rem(iz + n, gz), act)
                return 0
            lax.fori_loop(1, gz, step, 0)
        plane_of_others(iz, act)

    xs = (0, 1) if nbx == 2 else (0, 1, -1)
    ys = (0, 1, -1)

    def at_offset(ox, oy, oz):
        return device(lax.rem(ix + ox + gx, gx), lax.rem(iy + oy + gy, gy), lax.rem(iz + oz + gz, gz))

    barrier = pltpu.get_barrier_semaphore()

    def greet(to):
        pl.semaphore_signal(barrier, inc=1, device_id=to, device_id_type=MESH)

    per_plane = len(xs) * len(ys)
    if staged:
        @pl.when(iz < last)
        def _():
            whole_plane(last, greet)
            for ox in xs:
                for oy in ys:
                    if ox or oy:
                        greet(at_offset(ox, oy, 0))

        @pl.when(iz == last)
        def _():
            plane_of_others(iz, greet)

        @pl.when(iz + 1 < last)
        def _():
            for ox in xs:
                for oy in ys:
                    greet(at_offset(ox, oy, 1))
    else:
        each_other(greet)

    lane = lax.broadcasted_iota(jnp.int32, (2 * X, LANES), 1)
    slot_word = (lane * 10923) >> 17
    column = lane - STRIP * slot_word

    for load in loads[2:]:
        load.wait()
    if staged:
        @pl.when(iz == last)
        def _():
            pl.semaphore_wait(barrier, total - 1)

        @pl.when(iz == 0)
        def _():
            pl.semaphore_wait(barrier, per_plane - 1)

        @pl.when((iz > 0) & (iz < last))
        def _():
            pl.semaphore_wait(barrier, 2 * per_plane - 1)
    else:
        pl.semaphore_wait(barrier, total - 1)

    slot_of = {0: 0, 1: nbx - 1, -1: 1}
    groups = {"far": [], "near": [], 1: [], -1: []}
    split = {name: 0 for name in groups}
    count = 0
    for oz in (0, 1, -1):
        for ox in xs:
            for oy in ys:
                if ox == 0 and oz == 0 and oy == 0:
                    continue
                s = slot_of[ox]
                moves = []
                if oy == 0:
                    src_w, dst_w = {0: (pl.ds(1, W), pl.ds(1, W)), 1: (pl.ds(W, 1), pl.ds(0, 1)),
                                    -1: (pl.ds(1, 1), pl.ds(W + 1, 1))}[oz]
                    for f in range(2):
                        moves.append((words.at[f, pl.ds(0, X), src_w], words.at[f, pl.ds(s * X, X), dst_w]))
                moves.append((packs.at[0, 1, 1], packs.at[s, 1 - oz, 1 - oy]))
                for n, (src, dst) in enumerate(moves):
                    group = oz if oz else ("far" if ox else "near")
                    place = split[group] if n < len(moves) - 1 else len(groups[group])
                    split[group] += n < len(moves) - 1
                    groups[group].insert(place, pltpu.make_async_remote_copy(
                        src_ref=src, dst_ref=dst, send_sem=send_sem.at[count], recv_sem=recv_sem.at[count],
                        device_id=at_offset(ox, oy, oz), device_id_type=MESH))
                    count += 1

    def start(copies):
        for copy in copies:
            copy.start()

    def tell(semaphore, to):
        pl.semaphore_signal(semaphore, inc=1, device_id=to, device_id_type=MESH)

    def first_of(group):
        return groups[group][:split[group]]

    def rest_of(group):
        return groups[group][split[group]:]

    if staged:
        start(first_of("far"))

        @pl.when(iz == last)
        def _():
            start(first_of(1))

        @pl.when(iz > 0)
        def _():
            start(first_of(-1))
    else:
        for group in ("far", 1, -1):
            start(first_of(group))

    for load in loads[:2]:
        load.wait()
    pack = jnp.zeros((2 * X, LANES), jnp.int32)
    for w in range(W):
        rows = jnp.concatenate([p_ref[:, w, :], d_ref[:, w, :]], axis=0)
        base = STRIP * (w + 1)
        first = pltpu.roll(rows, (base - (LANES - 3)) % LANES, 1)
        second = pltpu.roll(rows, (base + 5 - (LANES - 2)) % LANES, 1)
        pack = jnp.where(slot_word == w + 1, jnp.where(column < 5, first, second), pack)
    packs[0, 1, 1] = pack

    if staged:
        @pl.when(iz == last)
        def _():
            start(rest_of(1))

        start(rest_of("far"))

        @pl.when(iz > 0)
        def _():
            start(rest_of(-1))

        start(groups["near"])

        @pl.when(iz > 0)
        def _():
            for ox in xs:
                for oy in ys:
                    tell(above, at_offset(ox, oy, -1))

        @pl.when(iz == last)
        def _():
            for z in range(last):
                tell(entered, device(ix, iy, z))
    else:
        for group in (1, "far", -1, "near"):
            start(rest_of(group))

    e_mul = disorder_width / LEVELS
    e_add = disorder_width * (0.5 / LEVELS - 0.5)
    two_mul = 2.0 / (spectral_scale * spectral_scale)
    three_mul = 2.0 / spectral_scale
    one_mul = 1.0 / spectral_scale
    probe = lax.broadcasted_iota(jnp.int32, (PROBES, LANES), 0)
    lane8 = lax.broadcasted_iota(jnp.int32, (PROBES, LANES), 1)
    slot8 = (lane8 * 10923) >> 17
    col8 = lane8 - STRIP * slot8
    lifts = [31 - (SITES * probe + j) for j in range(SITES)]
    zero = jnp.zeros((PROBES, LANES), jnp.float32)

    def sign_of(row, j):
        return jnp.where((jnp.broadcast_to(row, (PROBES, LANES)) << lifts[j]) < 0, 1.0, -1.0).astype(jnp.float32)

    def energy_of(row, j):
        level = (jnp.broadcast_to(row, (PROBES, LANES)) >> (8 * j)) & 255
        return level.astype(jnp.float32) * e_mul + e_add

    def unpack(q, zs):
        for z in zs:
            w, j = divmod(z + SITES, SITES)
            v0[q, z + SITES] = sign_of(words[0, q, w], j)
            en[q, z + SITES] = energy_of(words[1, q, w], j)

    def plane(e):
        return lax.rem(e + M, M)

    def planes(low, high, body):
        def step(i, _):
            body(plane(i - low))
            return 0
        lax.fori_loop(0, min(M, X + low + high), step, 0)

    def join_strips(s, oz):
        return jnp.where(column < 3, packs[s, oz, 0], jnp.where(column < 7, packs[s, oz, 1], packs[s, oz, 2]))

    def place_strips(s, oz):
        joined = join_strips(s, oz)
        own = pl.ds(s * X, X)
        side_slot = {0: 0, 1: None, 2: W + 1}[oz]
        move = {0: -STRIP * W, 1: 0, 2: STRIP * W}[oz]

        def put(ref, at, turn):
            value = pltpu.roll(joined, (move + turn) % LANES, 1) if move + turn else joined
            if side_slot is not None:
                base = STRIP * side_slot + turn
                value = jnp.where((lane >= base) & (lane < base + STRIP), value, ref[at])
            ref[at] = value

        put(strips, s, 0)
        for n, turn in enumerate((-1, 1, -STRIP, STRIP)):
            put(turned, (s, n), turn)
        signs = joined[:X]
        for w in range(1, W + 1) if oz == 1 else [side_slot]:
            rows = words[0, own, w, 0, :]
            below = pltpu.roll(signs, (move - STRIP * w - 2) % LANES, 1)
            above_it = pltpu.roll(signs, (move - STRIP * w - 8) % LANES, 1)
            rights[own, w, 0, :] = jnp.where(lane[:X] == LANES - 1, above_it, pltpu.roll(rows, LANES - 1, 1))
            lefts[own, w, 0, :] = jnp.where(lane[:X] == 0, below, pltpu.roll(rows, 1, 1))

    def unpack_strips(s):
        for x in range(X):
            for j in range(SITES):
                s0[s * X + x, j] = sign_of(strips[s, x:x + 1], j)
                se[s * X + x, j] = energy_of(strips[s, X + x:X + x + 1], j)

    def strip_one(q):
        s, x = divmod(q, X)
        for j in range(SITES):
            right, left, z_up, z_down = (turned[s, n, x:x + 1] for n in range(4))
            mine = s0[q, j]
            six = (s0[(q + 1) % M, j] + s0[(q + M - 1) % M, j] + sign_of(right, j) + sign_of(left, j)
                   + (s0[q, j + 1] if j + 1 < SITES else sign_of(z_up, 0))
                   + (s0[q, j - 1] if j > 0 else sign_of(z_down, SITES - 1)))
            new = se[q, j] * mine - six
            s1[q, j] = new
            g1[q, j] = edge_of(new)

    def strips_one():
        for q in sorted({e % M for e in range(-1, X + 1)}):
            strip_one(q)

    def strip_sum(src, q, up, down):
        mine = [src[q, j] for j in range(SITES)]
        sums, rights, ups = [], [], []
        for j in range(SITES):
            z_up = mine[j + 1] if j + 1 < SITES else pltpu.roll(mine[0], LANES - STRIP, 1)
            z_down = mine[j - 1] if j > 0 else pltpu.roll(mine[SITES - 1], STRIP, 1)
            sums.append(src[up, j] + src[down, j] + pltpu.roll(mine[j], LANES - 1, 1)
                        + pltpu.roll(mine[j], 1, 1) + z_up + z_down)
        return mine, sums

    def edge_of(tile):
        return jnp.where(col8 == 1, pltpu.roll(tile, LANES - 6, 1), tile)

    def site_sum(src, q, up, down, z, edges):
        w, j = divmod(z + SITES, SITES)
        fix = pltpu.roll(edges[q, j], (-(STRIP * w + 2)) % LANES, 1)
        mid = src[q, z + SITES]
        right = jnp.where(lane8 == LANES - 1, fix, pltpu.roll(mid, LANES - 1, 1))
        left = jnp.where(lane8 == 0, fix, pltpu.roll(mid, 1, 1))
        return mid, src[up, z + SITES] + src[down, z + SITES] + right + left + src[q, z + SITES + 1] + src[q, z + SITES - 1]

    def around_plane(e):
        return plane(e), plane(e + 1), plane(e + M - 1)

    def level_one(e, zs):
        q, up, down = around_plane(e)
        for z in zs:
            w, j = divmod(z + SITES, SITES)
            at = z + SITES
            total_six = (v0[up, at] + v0[down, at] + sign_of(rights[q, w], j) + sign_of(lefts[q, w], j)
                         + v0[q, at + 1] + v0[q, at - 1])
            v1[q, at] = en[q, at] * v0[q, at] - total_six

    def level_two(e, zs):
        q, up, down = around_plane(e)
        for z in zs:
            mid, total_six = site_sum(v1, q, up, down, z, g1)
            v2[q, z + SITES] = two_mul * (en[q, z + SITES] * mid - total_six) - v0[q, z + SITES]

    slot8 = (lane8 * 10923) >> 17

    def moments_of(x, zs, sums):
        q, up, down = around_plane(x)
        one, two, three = sums
        pair, rim = zero, zero
        for z in zs:
            at = z + SITES
            mid = v1[q, at]
            square = mid * mid
            one, two = one + v0[q, at] * mid, two + square
            three = three + en[q, at] * square - mid * (v1[up, at] + v1[down, at] + v1[q, at + 1] + v1[q, at - 1])
            pair = pair + mid * pltpu.roll(mid, LANES - 1, 1)
        for j in range(SITES):
            z_at = SITES * (slot8 - 1) + j
            mine = s1[q, j]
            seam = ((col8 == 2) | (col8 == 6)) & (z_at >= min(zs)) & (z_at <= max(zs))
            rim = rim + jnp.where(seam, mine * pltpu.roll(mine, LANES - 1, 1), 0.0)
        return one, two, three - rim - jnp.where(lane8 < LANES - 1, 2.0 * pair, 0.0)

    def strips_two():
        for q in range(X):
            mine, six = strip_sum(s1, q, q + 1, (q + M - 1) % M)
            for j in range(SITES):
                g2[q, j] = edge_of(two_mul * (se[q, j] * mine[j] - six[j]) - s0[q, j])

    def level_three(x, zs):
        q, up, down = around_plane(x)
        for z in zs:
            mid, total_six = site_sum(v2, q, up, down, z, g2)
            new = three_mul * (en[q, z + SITES] * mid - total_six) - one_mul * v1[q, z + SITES]
            at = pl.ds(x * Z + z, PROBES, stride=X * Z + PAD)
            prev_ref[at, :] = mid
            cur_ref[at, :] = new

    def loop(low, high, body):
        def step(i, _):
            body(i)
            return 0
        lax.fori_loop(low, high, step, 0)

    def own_moments(zs):
        sums = (zero, zero, zero)
        for x in range(X):
            sums = moments_of(x, zs, sums)
        return sums

    def send_moments(sums):
        row = zero
        for n, acc in enumerate(sums):
            summed = jnp.broadcast_to(jnp.sum(acc, axis=1, keepdims=True), (PROBES, LANES))
            row = row + jnp.where(lane8 == PROBES * n + probe, summed, 0.0)
        moms[me] = jnp.sum(row, axis=0, keepdims=True)
        each_other(lambda to: pltpu.make_async_remote_copy(
            src_ref=moms.at[me], dst_ref=moms.at[me], send_sem=msend_sem, recv_sem=mrecv_sem,
            device_id=to, device_id_type=MESH).start())

    def unpack_own(x, _):
        unpack(x, range(Z))
        return 0

    def unpack_far(i, _):
        unpack(plane(X + i), range(Z))
        return 0

    def unpack_low(i, _):
        unpack(plane(i - 3), range(Z))
        return 0

    lax.fori_loop(0, X, unpack_own, 0)
    for copy in groups["near"]:
        copy.wait_recv()
    place_strips(0, 1)
    unpack_strips(0)
    main = range(1, Z - 1)
    loop(1, X - 1, lambda x: level_one(x, main))
    for copy in groups["far"]:
        copy.wait_recv()
    for s in range(1, nbx):
        place_strips(s, 1)
        unpack_strips(s)
    if M <= X + 6:
        lax.fori_loop(0, M - X, unpack_far, 0)
    else:
        lax.fori_loop(0, 3, unpack_far, 0)
        lax.fori_loop(0, 3, unpack_low, 0)

    if staged:
        @pl.when(iz < last)
        def _():
            pl.semaphore_wait(above, per_plane)
            start(groups[1])

    def ends_of(low):
        width = X - 1 - 2 * low

        def body(i):
            level_one(low + i * width, main)
        return body

    strips_one()
    loop(0, 2, ends_of(0))
    loop(0, 2, ends_of(-1))
    middle = range(2, Z - 2)
    sums = lax.fori_loop(0, X, lambda x, sums: moments_of(x, middle, sums), (zero, zero, zero))
    for n in range(3):
        accs[n] = sums[n]

    def middle_rows():
        loop(0, X, lambda x: level_two(x, middle))
        loop(0, min(M, X + 4) - (X + 2), ends_of(-2))

    @pl.when(iz == last)
    def _():
        send_moments([accs[n] for n in range(3)])
        middle_rows()

    def side(up):
        for copy in groups[-1 if up else 1]:
            copy.wait_recv()
        outside = range(Z, Z + SITES) if up else range(-SITES, 0)
        planes(3, 3, lambda q: unpack(q, outside))
        for s in range(nbx):
            place_strips(s, 2 if up else 0)
            unpack_strips(s)
        ones = range(Z - 1, Z + 3) if up else range(-3, 1)
        twos = range(Z - 2, Z + 2) if up else range(-2, 2)
        strips_one()
        loop(0, X + 2, lambda i: level_one(i - 1, ones))
        sums = own_moments(twos)
        on = (iz != last) if up else (iz == 0)
        for n in range(3):
            accs[n] = accs[n] + jnp.where(on, sums[n], 0.0)

        if up:
            @pl.when((iz > 0) & (iz < last))
            def _():
                if staged:
                    pl.semaphore_wait(entered, 1)
                send_moments([accs[n] for n in range(3)])

            @pl.when(iz < last)
            def _():
                middle_rows()
        else:
            @pl.when(iz == 0)
            def _():
                send_moments([accs[n] for n in range(3)])

        outer = range(Z - 1, Z) if up else range(1)
        loop(0, min(M, X + 4) - (X + 2), lambda i: level_one(i * (X + 3) - 2, outer))

    def finish(twos, zs):
        loop(0, X, lambda x: level_two(x, twos))
        loop(0, 2, lambda i: level_two(i * (X + 1) - 1, zs))
        strips_two()
        loop(0, X, lambda x: level_three(x, zs))

    bottom, top = [-1, 0, 1], [Z - 2, Z - 1, Z]

    @pl.when(iz == last)
    def _():
        side(False)
        finish(bottom, range(Z - 3))

    if staged:
        @pl.when(iz == 0)
        def _():
            pl.semaphore_wait(entered, 1)
            start(groups[-1])

    side(True)

    @pl.when(iz == last)
    def _():
        finish(top, range(Z - 3, Z))

    @pl.when(iz < last)
    def _():
        side(False)
        finish(bottom + top, range(Z))

    for group in groups.values():
        for copy in group:
            copy.wait_send()
    others = moms.at[pl.ds(0, total - 1)]
    pltpu.make_async_copy(others, others, msend_sem).wait()
    sites = total * X * Z * LANES
    pltpu.make_async_copy(others, others, mrecv_sem).wait()
    sums = jnp.sum(moms[...], axis=0) * (1.0 / sites)
    first = one_mul * sums
    second = two_mul * pltpu.roll(sums, LANES - PROBES, 1) - 1.0
    third = (three_mul * two_mul) * pltpu.roll(sums, LANES - 2 * PROBES, 1) - 3.0 * first
    mom_ref[...] = jnp.concatenate([first, second, third], axis=0)[:, :PROBES]


def write_out(mom_ref, prev_ref, cur_ref, mom_hbm, prev_hbm, cur_hbm, sem):
    rows = prev_hbm.shape[1]
    inner = pl.ds(0, rows)
    copies = [pltpu.make_async_copy(src, dst, sem.at[n]) for n, (src, dst) in enumerate((
        (prev_ref.at[:, inner], prev_hbm), (cur_ref.at[:, inner], cur_hbm), (mom_ref, mom_hbm)))]
    for copy in copies:
        copy.start()
    for copy in copies:
        copy.wait()


def per_device(names, sizes, probe_bits, disorder_levels):
    X, W, Y = probe_bits.shape
    if Y != LANES or STRIP * (W + 2) > LANES or X < 3:
        raise ValueError("block size")
    Z = SITES * W
    nbx = 2 if sizes["gx"] == 2 else 3
    M = nbx * X
    n_copies = (9 * nbx - 1) + 2 * (3 * nbx - 1)
    total = sizes["gx"] * sizes["gy"] * sizes["gz"]
    rows = (X, W, 1, Y)
    vmem = pl.BlockSpec(memory_space=pltpu.VMEM)
    f32, i32 = jnp.float32, jnp.int32
    tile = (PROBES, LANES)
    hbm = pl.BlockSpec(memory_space=pltpu.HBM)
    out_shape = (
        jax.ShapeDtypeStruct((3, PROBES), f32),
        jax.ShapeDtypeStruct((PROBES, X * Z, Y), f32),
        jax.ShapeDtypeStruct((PROBES, X * Z, Y), f32),
    )
    padded = jax.ShapeDtypeStruct((PROBES * (X * Z + PAD), Y), f32)
    padded_shape = (out_shape[0], padded, padded)
    results = pl.pallas_call(
        functools.partial(kernel, names, sizes),
        out_shape=padded_shape,
        in_specs=[hbm] * 4,
        out_specs=(vmem,) * 3,
        scratch_shapes=[
            pltpu.VMEM((X, W, Y), i32),
            pltpu.VMEM((X, W, Y), i32),
            pltpu.VMEM((2, M, W + 2, 1, LANES), i32),
            pltpu.VMEM((M, W + 2, 1, LANES), i32),
            pltpu.VMEM((M, W + 2, 1, LANES), i32),
            pltpu.VMEM((nbx, 3, 3, 2 * X, LANES), i32),
            pltpu.VMEM((nbx, 2 * X, LANES), i32),
            pltpu.VMEM((M, Z + 2 * SITES) + tile, f32),
            pltpu.VMEM((M, Z + 2 * SITES) + tile, f32),
            pltpu.VMEM((M, Z + 2 * SITES) + tile, f32),
            pltpu.VMEM((M, Z + 2 * SITES) + tile, f32),
            pltpu.VMEM((M, SITES) + tile, f32),
            pltpu.VMEM((M, SITES) + tile, f32),
            pltpu.VMEM((M, SITES) + tile, f32),
            pltpu.VMEM((M, SITES) + tile, f32),
            pltpu.VMEM((M, SITES) + tile, f32),
            pltpu.VMEM((nbx, 4, 2 * X, LANES), i32),
            pltpu.VMEM((3,) + tile, f32),
            pltpu.VMEM((total, 1, LANES), f32),
            pltpu.SemaphoreType.DMA((4,)),
            pltpu.SemaphoreType.DMA((n_copies,)),
            pltpu.SemaphoreType.DMA((n_copies,)),
            pltpu.SemaphoreType.DMA,
            pltpu.SemaphoreType.DMA,
            pltpu.SemaphoreType.REGULAR,
            pltpu.SemaphoreType.REGULAR,
        ],
        compiler_params=pltpu.CompilerParams(collective_id=0, has_side_effects=True,
                                             vmem_limit_bytes=40 * 1024 * 1024),
    )(*[pltpu.with_memory_space_constraint(a, pltpu.HBM) for a in (probe_bits, disorder_levels, probe_bits.reshape(rows), disorder_levels.reshape(rows))])
    moments, previous, current = pl.pallas_call(
        write_out,
        out_shape=out_shape,
        in_specs=[vmem] * 3,
        out_specs=(hbm,) * 3,
        scratch_shapes=[pltpu.SemaphoreType.DMA((3,))],
        compiler_params=pltpu.CompilerParams(vmem_limit_bytes=16 * 1024 * 1024),
    )(results[0], *[a.reshape(PROBES, X * Z + PAD, Y) for a in results[1:]])
    shape = (PROBES, X, Z, Y)
    return moments, previous.reshape(shape), current.reshape(shape)


def solution(mesh):
    placed = (P("gx", "gz", "gy"), P("gx", "gz", "gy"))
    sizes = {a: mesh.shape[a] for a in mesh.axis_names}
    return jax.shard_map(
        functools.partial(per_device, tuple(mesh.axis_names), sizes),
        mesh=mesh,
        in_specs=placed,
        out_specs=(P(), P(None, "gx", "gz", "gy"), P(None, "gx", "gz", "gy")),
        check_vma=False,
    )
```

```python
import functools

import jax
import jax.numpy as jnp
from jax import lax
from jax.experimental import pallas as pl
from jax.experimental.pallas import tpu as pltpu
from jax.sharding import PartitionSpec as P

PROBES = 8
LEVELS = 256
LANES = 128
SITES = 4
STRIP = 12
PAD = 8

disorder_width = 4.0
spectral_scale = 8.4
MESH = pl.DeviceIdType.MESH


def kernel(names, sizes, p_hbm, d_hbm, prow_hbm, drow_hbm, mom_ref, prev_ref, cur_ref,
           p_ref, d_ref, words, lefts, rights, packs, strips, v0, v1, v2, en, s0, s1, se, g1, g2, turned, accs, moms,
           load_sem, send_sem, recv_sem, msend_sem, mrecv_sem, above, entered):
    X, W, _ = p_ref.shape
    Z = SITES * W
    nbx = packs.shape[0]
    M = nbx * X
    gx, gy, gz = sizes["gx"], sizes["gy"], sizes["gz"]
    ix, iy, iz = (lax.axis_index(a) for a in ("gx", "gy", "gz"))
    total = gx * gy * gz
    me = (ix * gy + iy) * gz + iz
    last = gz - 1
    staged = gx <= 3 and gy <= 4 and 3 <= gz <= 4

    def device(x, y, z):
        at = {"gx": x, "gy": y, "gz": z}
        return tuple(at[a] for a in names)

    loads = [pltpu.make_async_copy(src, dst, load_sem.at[n]) for n, (src, dst) in enumerate((
        (p_hbm, p_ref), (d_hbm, d_ref),
        (prow_hbm, words.at[0, pl.ds(0, X), pl.ds(1, W)]), (drow_hbm, words.at[1, pl.ds(0, X), pl.ds(1, W)])))]
    for load in loads:
        load.start()

    def around(at, size):
        steps = [at]
        for _ in range(size - 1):
            steps.append(jnp.where(steps[-1] + 1 == size, 0, steps[-1] + 1))
        return steps

    around_x, around_y = around(ix, gx), around(iy, gy)

    def plane_of_others(z, act):
        for x in range(gx):
            for y in range(gy):
                if x or y:
                    act(device(around_x[x], around_y[y], z))

    def whole_plane(z, act):
        for x in range(gx):
            for y in range(gy):
                act(device(around_x[x], around_y[y], z))

    def each_other(act):
        if gz <= 4:
            for z in range(gz):
                @pl.when(iz != z)
                def _(z=z):
                    whole_plane(z, act)
        else:
            def step(n, _):
                whole_plane(lax.rem(iz + n, gz), act)
                return 0
            lax.fori_loop(1, gz, step, 0)
        plane_of_others(iz, act)

    xs = (0, 1) if nbx == 2 else (0, 1, -1)
    ys = (0, 1, -1)

    def at_offset(ox, oy, oz):
        return device(lax.rem(ix + ox + gx, gx), lax.rem(iy + oy + gy, gy), lax.rem(iz + oz + gz, gz))

    barrier = pltpu.get_barrier_semaphore()

    def greet(to):
        pl.semaphore_signal(barrier, inc=1, device_id=to, device_id_type=MESH)

    per_plane = len(xs) * len(ys)
    if staged:
        for ox in xs:
            for oy in ys:
                if ox or oy:
                    greet(at_offset(ox, oy, 0))

        @pl.when(iz < last)
        def _():
            whole_plane(last, greet)

        @pl.when(iz + 1 < last)
        def _():
            for ox in xs:
                for oy in ys:
                    greet(at_offset(ox, oy, 1))
    else:
        each_other(greet)

    lane = lax.broadcasted_iota(jnp.int32, (2 * X, LANES), 1)
    slot_word = (lane * 10923) >> 17
    column = lane - STRIP * slot_word

    for load in loads[2:]:
        load.wait()
    if staged:
        @pl.when(iz == last)
        def _():
            pl.semaphore_wait(barrier, total - 1 - (gx * gy - per_plane))

        @pl.when(iz == 0)
        def _():
            pl.semaphore_wait(barrier, per_plane - 1)

        @pl.when((iz > 0) & (iz < last))
        def _():
            pl.semaphore_wait(barrier, 2 * per_plane - 1)
    else:
        pl.semaphore_wait(barrier, total - 1)

    slot_of = {0: 0, 1: nbx - 1, -1: 1}
    groups = {"far": [], "near": [], 1: [], -1: []}
    split = {name: 0 for name in groups}
    count = 0
    for oz in (0, 1, -1):
        for ox in xs:
            for oy in ys:
                if ox == 0 and oz == 0 and oy == 0:
                    continue
                s = slot_of[ox]
                moves = []
                if oy == 0:
                    src_w, dst_w = {0: (pl.ds(1, W), pl.ds(1, W)), 1: (pl.ds(W, 1), pl.ds(0, 1)),
                                    -1: (pl.ds(1, 1), pl.ds(W + 1, 1))}[oz]
                    for f in range(2):
                        moves.append((words.at[f, pl.ds(0, X), src_w], words.at[f, pl.ds(s * X, X), dst_w]))
                moves.append((packs.at[0, 1, 1], packs.at[s, 1 - oz, 1 - oy]))
                for n, (src, dst) in enumerate(moves):
                    group = oz if oz else ("far" if ox else "near")
                    place = split[group] if n < len(moves) - 1 else len(groups[group])
                    split[group] += n < len(moves) - 1
                    groups[group].insert(place, pltpu.make_async_remote_copy(
                        src_ref=src, dst_ref=dst, send_sem=send_sem.at[count], recv_sem=recv_sem.at[count],
                        device_id=at_offset(ox, oy, oz), device_id_type=MESH))
                    count += 1

    def start(copies):
        for copy in copies:
            copy.start()

    def tell(semaphore, to):
        pl.semaphore_signal(semaphore, inc=1, device_id=to, device_id_type=MESH)

    def first_of(group):
        return groups[group][:split[group]]

    def rest_of(group):
        return groups[group][split[group]:]

    if staged:
        start(first_of("far"))

        @pl.when(iz == last)
        def _():
            start(first_of(1))

        @pl.when(iz > 0)
        def _():
            start(first_of(-1))
    else:
        for group in ("far", 1, -1):
            start(first_of(group))

    for load in loads[:2]:
        load.wait()
    pack = jnp.zeros((2 * X, LANES), jnp.int32)
    for w in range(W):
        rows = jnp.concatenate([p_ref[:, w, :], d_ref[:, w, :]], axis=0)
        base = STRIP * (w + 1)
        first = pltpu.roll(rows, (base - (LANES - 3)) % LANES, 1)
        second = pltpu.roll(rows, (base + 5 - (LANES - 2)) % LANES, 1)
        pack = jnp.where(slot_word == w + 1, jnp.where(column < 5, first, second), pack)
    packs[0, 1, 1] = pack

    if staged:
        @pl.when(iz == last)
        def _():
            start(rest_of(1))

        start(rest_of("far"))

        @pl.when(iz > 0)
        def _():
            start(rest_of(-1))

        start(groups["near"])

        @pl.when(iz > 0)
        def _():
            for ox in xs:
                for oy in ys:
                    tell(above, at_offset(ox, oy, -1))

        @pl.when(iz == last)
        def _():
            for z in range(last - 1):
                for ox in xs:
                    for oy in ys:
                        tell(entered, at_offset(ox, oy, z + 1))
    else:
        for group in (1, "far", -1, "near"):
            start(rest_of(group))

    e_mul = disorder_width / LEVELS
    e_add = disorder_width * (0.5 / LEVELS - 0.5)
    two_mul = 2.0 / (spectral_scale * spectral_scale)
    three_mul = 2.0 / spectral_scale
    one_mul = 1.0 / spectral_scale
    probe = lax.broadcasted_iota(jnp.int32, (PROBES, LANES), 0)
    lane8 = lax.broadcasted_iota(jnp.int32, (PROBES, LANES), 1)
    slot8 = (lane8 * 10923) >> 17
    col8 = lane8 - STRIP * slot8
    lifts = [31 - (SITES * probe + j) for j in range(SITES)]
    zero = jnp.zeros((PROBES, LANES), jnp.float32)

    def sign_of(row, j):
        return jnp.where((jnp.broadcast_to(row, (PROBES, LANES)) << lifts[j]) < 0, 1.0, -1.0).astype(jnp.float32)

    def energy_of(row, j):
        level = (jnp.broadcast_to(row, (PROBES, LANES)) >> (8 * j)) & 255
        return level.astype(jnp.float32) * e_mul + e_add

    def unpack(q, zs):
        for z in zs:
            w, j = divmod(z + SITES, SITES)
            v0[q, z + SITES] = sign_of(words[0, q, w], j)
            en[q, z + SITES] = energy_of(words[1, q, w], j)

    def plane(e):
        return lax.rem(e + M, M)

    def planes(low, high, body):
        def step(i, _):
            body(plane(i - low))
            return 0
        lax.fori_loop(0, min(M, X + low + high), step, 0)

    def join_strips(s, oz):
        return jnp.where(column < 3, packs[s, oz, 0], jnp.where(column < 7, packs[s, oz, 1], packs[s, oz, 2]))

    def place_strips(s, oz):
        joined = join_strips(s, oz)
        own = pl.ds(s * X, X)
        side_slot = {0: 0, 1: None, 2: W + 1}[oz]
        move = {0: -STRIP * W, 1: 0, 2: STRIP * W}[oz]

        def put(ref, at, turn):
            value = pltpu.roll(joined, (move + turn) % LANES, 1) if move + turn else joined
            if side_slot is not None:
                base = STRIP * side_slot + turn
                value = jnp.where((lane >= base) & (lane < base + STRIP), value, ref[at])
            ref[at] = value

        put(strips, s, 0)
        for n, turn in enumerate((-1, 1, -STRIP, STRIP)):
            put(turned, (s, n), turn)
        signs = joined[:X]
        for w in range(1, W + 1) if oz == 1 else [side_slot]:
            rows = words[0, own, w, 0, :]
            below = pltpu.roll(signs, (move - STRIP * w - 2) % LANES, 1)
            above_it = pltpu.roll(signs, (move - STRIP * w - 8) % LANES, 1)
            rights[own, w, 0, :] = jnp.where(lane[:X] == LANES - 1, above_it, pltpu.roll(rows, LANES - 1, 1))
            lefts[own, w, 0, :] = jnp.where(lane[:X] == 0, below, pltpu.roll(rows, 1, 1))

    def unpack_strips(s):
        for x in range(X):
            for j in range(SITES):
                s0[s * X + x, j] = sign_of(strips[s, x:x + 1], j)
                se[s * X + x, j] = energy_of(strips[s, X + x:X + x + 1], j)

    def strip_one(q):
        s, x = divmod(q, X)
        for j in range(SITES):
            right, left, z_up, z_down = (turned[s, n, x:x + 1] for n in range(4))
            mine = s0[q, j]
            six = (s0[(q + 1) % M, j] + s0[(q + M - 1) % M, j] + sign_of(right, j) + sign_of(left, j)
                   + (s0[q, j + 1] if j + 1 < SITES else sign_of(z_up, 0))
                   + (s0[q, j - 1] if j > 0 else sign_of(z_down, SITES - 1)))
            new = se[q, j] * mine - six
            s1[q, j] = new
            g1[q, j] = edge_of(new)

    def strips_one():
        for q in sorted({e % M for e in range(-1, X + 1)}):
            strip_one(q)

    def strip_sum(src, q, up, down):
        mine = [src[q, j] for j in range(SITES)]
        sums, rights, ups = [], [], []
        for j in range(SITES):
            z_up = mine[j + 1] if j + 1 < SITES else pltpu.roll(mine[0], LANES - STRIP, 1)
            z_down = mine[j - 1] if j > 0 else pltpu.roll(mine[SITES - 1], STRIP, 1)
            sums.append(src[up, j] + src[down, j] + pltpu.roll(mine[j], LANES - 1, 1)
                        + pltpu.roll(mine[j], 1, 1) + z_up + z_down)
        return mine, sums

    def edge_of(tile):
        return jnp.where(col8 == 1, pltpu.roll(tile, LANES - 6, 1), tile)

    def site_sum(src, q, up, down, z, edges):
        w, j = divmod(z + SITES, SITES)
        fix = pltpu.roll(edges[q, j], (-(STRIP * w + 2)) % LANES, 1)
        mid = src[q, z + SITES]
        right = jnp.where(lane8 == LANES - 1, fix, pltpu.roll(mid, LANES - 1, 1))
        left = jnp.where(lane8 == 0, fix, pltpu.roll(mid, 1, 1))
        return mid, src[up, z + SITES] + src[down, z + SITES] + right + left + src[q, z + SITES + 1] + src[q, z + SITES - 1]

    def around_plane(e):
        return plane(e), plane(e + 1), plane(e + M - 1)

    def level_one(e, zs):
        q, up, down = around_plane(e)
        for z in zs:
            w, j = divmod(z + SITES, SITES)
            at = z + SITES
            total_six = (v0[up, at] + v0[down, at] + sign_of(rights[q, w], j) + sign_of(lefts[q, w], j)
                         + v0[q, at + 1] + v0[q, at - 1])
            v1[q, at] = en[q, at] * v0[q, at] - total_six

    def level_two(e, zs):
        q, up, down = around_plane(e)
        for z in zs:
            mid, total_six = site_sum(v1, q, up, down, z, g1)
            v2[q, z + SITES] = two_mul * (en[q, z + SITES] * mid - total_six) - v0[q, z + SITES]

    slot8 = (lane8 * 10923) >> 17

    def moments_of(x, zs, sums):
        q, up, down = around_plane(x)
        one, two, three = sums
        pair, rim = zero, zero
        for z in zs:
            at = z + SITES
            mid = v1[q, at]
            square = mid * mid
            one, two = one + v0[q, at] * mid, two + square
            three = three + en[q, at] * square - mid * (v1[up, at] + v1[down, at] + v1[q, at + 1] + v1[q, at - 1])
            pair = pair + mid * pltpu.roll(mid, LANES - 1, 1)
        for j in range(SITES):
            z_at = SITES * (slot8 - 1) + j
            mine = s1[q, j]
            seam = ((col8 == 2) | (col8 == 6)) & (z_at >= min(zs)) & (z_at <= max(zs))
            rim = rim + jnp.where(seam, mine * pltpu.roll(mine, LANES - 1, 1), 0.0)
        return one, two, three - rim - jnp.where(lane8 < LANES - 1, 2.0 * pair, 0.0)

    def strips_two():
        for q in range(X):
            mine, six = strip_sum(s1, q, q + 1, (q + M - 1) % M)
            for j in range(SITES):
                g2[q, j] = edge_of(two_mul * (se[q, j] * mine[j] - six[j]) - s0[q, j])

    def level_three(x, zs):
        q, up, down = around_plane(x)
        for z in zs:
            mid, total_six = site_sum(v2, q, up, down, z, g2)
            new = three_mul * (en[q, z + SITES] * mid - total_six) - one_mul * v1[q, z + SITES]
            at = pl.ds(x * Z + z, PROBES, stride=X * Z + PAD)
            prev_ref[at, :] = mid
            cur_ref[at, :] = new

    def loop(low, high, body):
        def step(i, _):
            body(i)
            return 0
        lax.fori_loop(low, high, step, 0)

    def own_moments(zs):
        sums = (zero, zero, zero)
        for x in range(X):
            sums = moments_of(x, zs, sums)
        return sums

    def send_moments(sums):
        row = zero
        for n, acc in enumerate(sums):
            summed = jnp.broadcast_to(jnp.sum(acc, axis=1, keepdims=True), (PROBES, LANES))
            row = row + jnp.where(lane8 == PROBES * n + probe, summed, 0.0)
        moms[me] = jnp.sum(row, axis=0, keepdims=True)
        each_other(lambda to: pltpu.make_async_remote_copy(
            src_ref=moms.at[me], dst_ref=moms.at[me], send_sem=msend_sem, recv_sem=mrecv_sem,
            device_id=to, device_id_type=MESH).start())

    def unpack_own(x, _):
        unpack(x, range(Z))
        return 0

    def unpack_far(i, _):
        unpack(plane(X + i), range(Z))
        return 0

    def unpack_low(i, _):
        unpack(plane(i - 3), range(Z))
        return 0

    lax.fori_loop(0, X, unpack_own, 0)
    for copy in groups["near"]:
        copy.wait_recv()
    place_strips(0, 1)
    unpack_strips(0)
    main = range(1, Z - 1)
    loop(1, X - 1, lambda x: level_one(x, main))
    for copy in groups["far"]:
        copy.wait_recv()
    for s in range(1, nbx):
        place_strips(s, 1)
        unpack_strips(s)
    strips_one()
    if M <= X + 6:
        lax.fori_loop(0, M - X, unpack_far, 0)
    else:
        lax.fori_loop(0, 3, unpack_far, 0)
        lax.fori_loop(0, 3, unpack_low, 0)

    if staged:
        @pl.when(iz < last)
        def _():
            pl.semaphore_wait(above, per_plane)
            start(groups[1])

    def ends_of(low):
        width = X - 1 - 2 * low

        def body(i):
            level_one(low + i * width, main)
        return body

    loop(0, 2, ends_of(0))
    loop(0, 2, ends_of(-1))
    middle = range(2, Z - 2)
    sums = lax.fori_loop(0, X // 2, lambda i, sums: moments_of(2 * i + 1, middle, moments_of(2 * i, middle, sums)),
                         (zero, zero, zero))
    if X % 2:
        sums = moments_of(X - 1, middle, sums)
    for n in range(3):
        accs[n] = sums[n]

    def middle_rows():
        loop(0, X, lambda x: level_two(x, middle))
        loop(0, min(M, X + 4) - (X + 2), ends_of(-2))

    @pl.when(iz == last)
    def _():
        send_moments([accs[n] for n in range(3)])
        middle_rows()

    def side(up):
        for copy in groups[-1 if up else 1]:
            copy.wait_recv()
        outside = range(Z, Z + SITES) if up else range(-SITES, 0)
        planes(3, 3, lambda q: unpack(q, outside))
        for s in range(nbx):
            place_strips(s, 2 if up else 0)
            unpack_strips(s)
        ones = range(Z - 1, Z + 3) if up else range(-3, 1)
        twos = range(Z - 2, Z + 2) if up else range(-2, 2)
        strips_one()
        loop(0, X + 2, lambda i: level_one(i - 1, ones))
        sums = own_moments(twos)
        on = (iz != last) if up else (iz == 0)
        for n in range(3):
            accs[n] = accs[n] + jnp.where(on, sums[n], 0.0)

        if up:
            @pl.when((iz > 0) & (iz < last))
            def _():
                if staged:
                    @pl.when(iz < last - 1)
                    def _():
                        pl.semaphore_wait(entered, per_plane)
                send_moments([accs[n] for n in range(3)])

            @pl.when(iz < last)
            def _():
                middle_rows()
        else:
            @pl.when(iz == 0)
            def _():
                send_moments([accs[n] for n in range(3)])

        outer = range(Z - 1, Z) if up else range(1)
        loop(0, min(M, X + 4) - (X + 2), lambda i: level_one(i * (X + 3) - 2, outer))

    def finish(twos, zs):
        loop(0, X, lambda x: level_two(x, twos))
        loop(0, 2, lambda i: level_two(i * (X + 1) - 1, zs))
        strips_two()
        loop(0, X, lambda x: level_three(x, zs))

    bottom, top = [-1, 0, 1], [Z - 2, Z - 1, Z]

    @pl.when(iz == last)
    def _():
        side(False)
        finish(bottom, range(Z - 3))

    if staged:
        @pl.when(iz == 0)
        def _():
            pl.semaphore_wait(entered, per_plane)
            start(groups[-1])

    side(True)

    @pl.when(iz == last)
    def _():
        finish(top, range(Z - 3, Z))

    @pl.when(iz < last)
    def _():
        side(False)
        finish(bottom + top, range(Z))

    for group in groups.values():
        for copy in group:
            copy.wait_send()
    others = moms.at[pl.ds(0, total - 1)]
    pltpu.make_async_copy(others, others, msend_sem).wait()
    sites = total * X * Z * LANES
    pltpu.make_async_copy(others, others, mrecv_sem).wait()
    sums = jnp.sum(moms[...], axis=0) * (1.0 / sites)
    first = one_mul * sums
    second = two_mul * pltpu.roll(sums, LANES - PROBES, 1) - 1.0
    third = (three_mul * two_mul) * pltpu.roll(sums, LANES - 2 * PROBES, 1) - 3.0 * first
    mom_ref[...] = jnp.concatenate([first, second, third], axis=0)[:, :PROBES]


def write_out(mom_ref, prev_ref, cur_ref, mom_hbm, prev_hbm, cur_hbm, sem):
    rows = prev_hbm.shape[1]
    inner = pl.ds(0, rows)
    copies = [pltpu.make_async_copy(src, dst, sem.at[n]) for n, (src, dst) in enumerate((
        (prev_ref.at[:, inner], prev_hbm), (cur_ref.at[:, inner], cur_hbm), (mom_ref, mom_hbm)))]
    for copy in copies:
        copy.start()
    for copy in copies:
        copy.wait()


def per_device(names, sizes, probe_bits, disorder_levels):
    X, W, Y = probe_bits.shape
    if Y != LANES or STRIP * (W + 2) > LANES or X < 3:
        raise ValueError("block size")
    Z = SITES * W
    nbx = 2 if sizes["gx"] == 2 else 3
    M = nbx * X
    n_copies = (9 * nbx - 1) + 2 * (3 * nbx - 1)
    total = sizes["gx"] * sizes["gy"] * sizes["gz"]
    rows = (X, W, 1, Y)
    vmem = pl.BlockSpec(memory_space=pltpu.VMEM)
    f32, i32 = jnp.float32, jnp.int32
    tile = (PROBES, LANES)
    hbm = pl.BlockSpec(memory_space=pltpu.HBM)
    out_shape = (
        jax.ShapeDtypeStruct((3, PROBES), f32),
        jax.ShapeDtypeStruct((PROBES, X * Z, Y), f32),
        jax.ShapeDtypeStruct((PROBES, X * Z, Y), f32),
    )
    padded = jax.ShapeDtypeStruct((PROBES * (X * Z + PAD), Y), f32)
    padded_shape = (out_shape[0], padded, padded)
    results = pl.pallas_call(
        functools.partial(kernel, names, sizes),
        out_shape=padded_shape,
        in_specs=[hbm] * 4,
        out_specs=(vmem,) * 3,
        scratch_shapes=[
            pltpu.VMEM((X, W, Y), i32),
            pltpu.VMEM((X, W, Y), i32),
            pltpu.VMEM((2, M, W + 2, 1, LANES), i32),
            pltpu.VMEM((M, W + 2, 1, LANES), i32),
            pltpu.VMEM((M, W + 2, 1, LANES), i32),
            pltpu.VMEM((nbx, 3, 3, 2 * X, LANES), i32),
            pltpu.VMEM((nbx, 2 * X, LANES), i32),
            pltpu.VMEM((M, Z + 2 * SITES) + tile, f32),
            pltpu.VMEM((M, Z + 2 * SITES) + tile, f32),
            pltpu.VMEM((M, Z + 2 * SITES) + tile, f32),
            pltpu.VMEM((M, Z + 2 * SITES) + tile, f32),
            pltpu.VMEM((M, SITES) + tile, f32),
            pltpu.VMEM((M, SITES) + tile, f32),
            pltpu.VMEM((M, SITES) + tile, f32),
            pltpu.VMEM((M, SITES) + tile, f32),
            pltpu.VMEM((M, SITES) + tile, f32),
            pltpu.VMEM((nbx, 4, 2 * X, LANES), i32),
            pltpu.VMEM((3,) + tile, f32),
            pltpu.VMEM((total, 1, LANES), f32),
            pltpu.SemaphoreType.DMA((4,)),
            pltpu.SemaphoreType.DMA((n_copies,)),
            pltpu.SemaphoreType.DMA((n_copies,)),
            pltpu.SemaphoreType.DMA,
            pltpu.SemaphoreType.DMA,
            pltpu.SemaphoreType.REGULAR,
            pltpu.SemaphoreType.REGULAR,
        ],
        compiler_params=pltpu.CompilerParams(collective_id=0, has_side_effects=True,
                                             vmem_limit_bytes=40 * 1024 * 1024),
    )(*[pltpu.with_memory_space_constraint(a, pltpu.HBM) for a in (probe_bits, disorder_levels, probe_bits.reshape(rows), disorder_levels.reshape(rows))])
    moments, previous, current = pl.pallas_call(
        write_out,
        out_shape=out_shape,
        in_specs=[vmem] * 3,
        out_specs=(hbm,) * 3,
        scratch_shapes=[pltpu.SemaphoreType.DMA((3,))],
        compiler_params=pltpu.CompilerParams(vmem_limit_bytes=16 * 1024 * 1024),
    )(results[0], *[a.reshape(PROBES, X * Z + PAD, Y) for a in results[1:]])
    shape = (PROBES, X, Z, Y)
    return moments, previous.reshape(shape), current.reshape(shape)


def solution(mesh):
    placed = (P("gx", "gz", "gy"), P("gx", "gz", "gy"))
    sizes = {a: mesh.shape[a] for a in mesh.axis_names}
    return jax.shard_map(
        functools.partial(per_device, tuple(mesh.axis_names), sizes),
        mesh=mesh,
        in_specs=placed,
        out_specs=(P(), P(None, "gx", "gz", "gy"), P(None, "gx", "gz", "gy")),
        check_vma=False,
    )
```

```python
import functools

import jax
import jax.numpy as jnp
from jax import lax
from jax.experimental import pallas as pl
from jax.experimental.pallas import tpu as pltpu
from jax.sharding import PartitionSpec as P

PROBES = 8
LEVELS = 256
LANES = 128
SITES = 4
STRIP = 12
PAD = 8

disorder_width = 4.0
spectral_scale = 8.4
MESH = pl.DeviceIdType.MESH


def kernel(names, sizes, p_hbm, d_hbm, prow_hbm, drow_hbm, mom_ref, prev_ref, cur_ref,
           p_ref, d_ref, words, lefts, rights, packs, strips, v0, v1, v2, en, s0, s1, se, g1, g2, turned, accs, moms,
           load_sem, send_sem, recv_sem, msend_sem, mrecv_sem, above, entered):
    X, W, _ = p_ref.shape
    Z = SITES * W
    nbx = packs.shape[0]
    M = nbx * X
    gx, gy, gz = sizes["gx"], sizes["gy"], sizes["gz"]
    ix, iy, iz = (lax.axis_index(a) for a in ("gx", "gy", "gz"))
    total = gx * gy * gz
    me = (ix * gy + iy) * gz + iz
    last = gz - 1
    staged = gx <= 3 and gy <= 4 and 3 <= gz <= 4

    def device(x, y, z):
        at = {"gx": x, "gy": y, "gz": z}
        return tuple(at[a] for a in names)

    loads = [pltpu.make_async_copy(src, dst, load_sem.at[n]) for n, (src, dst) in enumerate((
        (p_hbm, p_ref), (d_hbm, d_ref),
        (prow_hbm, words.at[0, pl.ds(0, X), pl.ds(1, W)]), (drow_hbm, words.at[1, pl.ds(0, X), pl.ds(1, W)])))]
    for load in loads:
        load.start()

    def around(at, size):
        steps = [at]
        for _ in range(size - 1):
            steps.append(jnp.where(steps[-1] + 1 == size, 0, steps[-1] + 1))
        return steps

    around_x, around_y = around(ix, gx), around(iy, gy)

    def plane_of_others(z, act):
        for x in range(gx):
            for y in range(gy):
                if x or y:
                    act(device(around_x[x], around_y[y], z))

    def whole_plane(z, act):
        for x in range(gx):
            for y in range(gy):
                act(device(around_x[x], around_y[y], z))

    def each_other(act):
        if gz <= 4:
            for z in range(gz):
                @pl.when(iz != z)
                def _(z=z):
                    whole_plane(z, act)
        else:
            def step(n, _):
                whole_plane(lax.rem(iz + n, gz), act)
                return 0
            lax.fori_loop(1, gz, step, 0)
        plane_of_others(iz, act)

    xs = (0, 1) if nbx == 2 else (0, 1, -1)
    ys = (0, 1, -1)

    def at_offset(ox, oy, oz):
        return device(lax.rem(ix + ox + gx, gx), lax.rem(iy + oy + gy, gy), lax.rem(iz + oz + gz, gz))

    barrier = pltpu.get_barrier_semaphore()

    def greet(to):
        pl.semaphore_signal(barrier, inc=1, device_id=to, device_id_type=MESH)

    per_plane = len(xs) * len(ys)
    if staged:
        for ox in xs:
            for oy in ys:
                if ox or oy:
                    greet(at_offset(ox, oy, 0))

        @pl.when(iz < last)
        def _():
            whole_plane(last, greet)

        @pl.when(iz + 1 < last)
        def _():
            for ox in xs:
                for oy in ys:
                    greet(at_offset(ox, oy, 1))
    else:
        each_other(greet)

    lane = lax.broadcasted_iota(jnp.int32, (2 * X, LANES), 1)
    slot_word = (lane * 10923) >> 17
    column = lane - STRIP * slot_word

    for load in loads[2:]:
        load.wait()
    if staged:
        @pl.when(iz == last)
        def _():
            pl.semaphore_wait(barrier, total - 1 - (gx * gy - per_plane))

        @pl.when(iz == 0)
        def _():
            pl.semaphore_wait(barrier, per_plane - 1)

        @pl.when((iz > 0) & (iz < last))
        def _():
            pl.semaphore_wait(barrier, 2 * per_plane - 1)
    else:
        pl.semaphore_wait(barrier, total - 1)

    slot_of = {0: 0, 1: nbx - 1, -1: 1}
    groups = {"far": [], "near": [], 1: [], -1: []}
    split = {name: 0 for name in groups}
    count = 0
    for oz in (0, 1, -1):
        for ox in xs:
            for oy in ys:
                if ox == 0 and oz == 0 and oy == 0:
                    continue
                s = slot_of[ox]
                moves = []
                if oy == 0:
                    src_w, dst_w = {0: (pl.ds(1, W), pl.ds(1, W)), 1: (pl.ds(W, 1), pl.ds(0, 1)),
                                    -1: (pl.ds(1, 1), pl.ds(W + 1, 1))}[oz]
                    for f in range(2):
                        moves.append((words.at[f, pl.ds(0, X), src_w], words.at[f, pl.ds(s * X, X), dst_w]))
                moves.append((packs.at[0, 1, 1], packs.at[s, 1 - oz, 1 - oy]))
                for n, (src, dst) in enumerate(moves):
                    group = oz if oz else ("far" if ox else "near")
                    place = split[group] if n < len(moves) - 1 else len(groups[group])
                    split[group] += n < len(moves) - 1
                    groups[group].insert(place, pltpu.make_async_remote_copy(
                        src_ref=src, dst_ref=dst, send_sem=send_sem.at[count], recv_sem=recv_sem.at[count],
                        device_id=at_offset(ox, oy, oz), device_id_type=MESH))
                    count += 1

    def start(copies):
        for copy in copies:
            copy.start()

    def tell(semaphore, to):
        pl.semaphore_signal(semaphore, inc=1, device_id=to, device_id_type=MESH)

    def first_of(group):
        return groups[group][:split[group]]

    def rest_of(group):
        return groups[group][split[group]:]

    if staged:
        start(first_of("far"))

        @pl.when(iz == last)
        def _():
            start(first_of(1))

        @pl.when(iz > 0)
        def _():
            start(first_of(-1))
    else:
        for group in ("far", 1, -1):
            start(first_of(group))

    for load in loads[:2]:
        load.wait()
    pack = jnp.zeros((2 * X, LANES), jnp.int32)
    for w in range(W):
        rows = jnp.concatenate([p_ref[:, w, :], d_ref[:, w, :]], axis=0)
        base = STRIP * (w + 1)
        first = pltpu.roll(rows, (base - (LANES - 3)) % LANES, 1)
        second = pltpu.roll(rows, (base + 5 - (LANES - 2)) % LANES, 1)
        pack = jnp.where(slot_word == w + 1, jnp.where(column < 5, first, second), pack)
    packs[0, 1, 1] = pack

    if staged:
        @pl.when(iz == last)
        def _():
            start(rest_of(1))

        start(rest_of("far"))

        @pl.when(iz > 0)
        def _():
            start(rest_of(-1))

        start(groups["near"])

        @pl.when(iz > 0)
        def _():
            for ox in xs:
                for oy in ys:
                    tell(above, at_offset(ox, oy, -1))

        @pl.when(iz == last)
        def _():
            for z in range(last - 1):
                for ox in xs:
                    for oy in ys:
                        tell(entered, at_offset(ox, oy, z + 1))
    else:
        for group in (1, "far", -1, "near"):
            start(rest_of(group))

    e_mul = disorder_width / LEVELS
    e_add = disorder_width * (0.5 / LEVELS - 0.5)
    two_mul = 2.0 / (spectral_scale * spectral_scale)
    three_mul = 2.0 / spectral_scale
    one_mul = 1.0 / spectral_scale
    probe = lax.broadcasted_iota(jnp.int32, (PROBES, LANES), 0)
    lane8 = lax.broadcasted_iota(jnp.int32, (PROBES, LANES), 1)
    slot8 = (lane8 * 10923) >> 17
    col8 = lane8 - STRIP * slot8
    lifts = [31 - (SITES * probe + j) for j in range(SITES)]
    zero = jnp.zeros((PROBES, LANES), jnp.float32)

    def sign_of(row, j):
        return jnp.where((jnp.broadcast_to(row, (PROBES, LANES)) << lifts[j]) < 0, 1.0, -1.0).astype(jnp.float32)

    def energy_of(row, j):
        level = (jnp.broadcast_to(row, (PROBES, LANES)) >> (8 * j)) & 255
        return level.astype(jnp.float32) * e_mul + e_add

    def unpack(q, zs):
        for z in zs:
            w, j = divmod(z + SITES, SITES)
            v0[q, z + SITES] = sign_of(words[0, q, w], j)
            en[q, z + SITES] = energy_of(words[1, q, w], j)

    def plane(e):
        return lax.rem(e + M, M)

    def planes(low, high, body):
        def step(i, _):
            body(plane(i - low))
            return 0
        lax.fori_loop(0, min(M, X + low + high), step, 0)

    def join_strips(s, oz):
        return jnp.where(column < 3, packs[s, oz, 0], jnp.where(column < 7, packs[s, oz, 1], packs[s, oz, 2]))

    def place_strips(s, oz):
        joined = join_strips(s, oz)
        own = pl.ds(s * X, X)
        side_slot = {0: 0, 1: None, 2: W + 1}[oz]
        move = {0: -STRIP * W, 1: 0, 2: STRIP * W}[oz]

        def put(ref, at, turn):
            value = pltpu.roll(joined, (move + turn) % LANES, 1) if move + turn else joined
            if side_slot is not None:
                base = STRIP * side_slot + turn
                value = jnp.where((lane >= base) & (lane < base + STRIP), value, ref[at])
            ref[at] = value

        put(strips, s, 0)
        for n, turn in enumerate((-1, 1, -STRIP, STRIP)):
            put(turned, (s, n), turn)
        signs = joined[:X]
        for w in range(1, W + 1) if oz == 1 else [side_slot]:
            rows = words[0, own, w, 0, :]
            below = pltpu.roll(signs, (move - STRIP * w - 2) % LANES, 1)
            above_it = pltpu.roll(signs, (move - STRIP * w - 8) % LANES, 1)
            rights[own, w, 0, :] = jnp.where(lane[:X] == LANES - 1, above_it, pltpu.roll(rows, LANES - 1, 1))
            lefts[own, w, 0, :] = jnp.where(lane[:X] == 0, below, pltpu.roll(rows, 1, 1))

    def unpack_strips(s):
        for x in range(X):
            for j in range(SITES):
                s0[s * X + x, j] = sign_of(strips[s, x:x + 1], j)
                se[s * X + x, j] = energy_of(strips[s, X + x:X + x + 1], j)

    def strip_one(q):
        s, x = divmod(q, X)
        for j in range(SITES):
            right, left, z_up, z_down = (turned[s, n, x:x + 1] for n in range(4))
            mine = s0[q, j]
            six = (s0[(q + 1) % M, j] + s0[(q + M - 1) % M, j] + sign_of(right, j) + sign_of(left, j)
                   + (s0[q, j + 1] if j + 1 < SITES else sign_of(z_up, 0))
                   + (s0[q, j - 1] if j > 0 else sign_of(z_down, SITES - 1)))
            new = se[q, j] * mine - six
            s1[q, j] = new
            g1[q, j] = edge_of(new)

    def strips_one():
        for q in sorted({e % M for e in range(-1, X + 1)}):
            strip_one(q)

    def strip_sum(src, q, up, down):
        mine = [src[q, j] for j in range(SITES)]
        sums, rights, ups = [], [], []
        for j in range(SITES):
            z_up = mine[j + 1] if j + 1 < SITES else pltpu.roll(mine[0], LANES - STRIP, 1)
            z_down = mine[j - 1] if j > 0 else pltpu.roll(mine[SITES - 1], STRIP, 1)
            sums.append(src[up, j] + src[down, j] + pltpu.roll(mine[j], LANES - 1, 1)
                        + pltpu.roll(mine[j], 1, 1) + z_up + z_down)
        return mine, sums

    def edge_of(tile):
        return jnp.where(col8 == 1, pltpu.roll(tile, LANES - 6, 1), tile)

    def site_sum(src, q, up, down, z, edges):
        w, j = divmod(z + SITES, SITES)
        fix = pltpu.roll(edges[q, j], (-(STRIP * w + 2)) % LANES, 1)
        mid = src[q, z + SITES]
        right = jnp.where(lane8 == LANES - 1, fix, pltpu.roll(mid, LANES - 1, 1))
        left = jnp.where(lane8 == 0, fix, pltpu.roll(mid, 1, 1))
        return mid, src[up, z + SITES] + src[down, z + SITES] + right + left + src[q, z + SITES + 1] + src[q, z + SITES - 1]

    def around_plane(e):
        return plane(e), plane(e + 1), plane(e + M - 1)

    def level_one(e, zs):
        q, up, down = around_plane(e)
        for z in zs:
            w, j = divmod(z + SITES, SITES)
            at = z + SITES
            total_six = (v0[up, at] + v0[down, at] + sign_of(rights[q, w], j) + sign_of(lefts[q, w], j)
                         + v0[q, at + 1] + v0[q, at - 1])
            v1[q, at] = en[q, at] * v0[q, at] - total_six

    def level_two(e, zs):
        q, up, down = around_plane(e)
        for z in zs:
            mid, total_six = site_sum(v1, q, up, down, z, g1)
            v2[q, z + SITES] = two_mul * (en[q, z + SITES] * mid - total_six) - v0[q, z + SITES]

    slot8 = (lane8 * 10923) >> 17

    def moments_of(x, zs, sums):
        q, up, down = around_plane(x)
        one, two, three = sums
        pair, rim = zero, zero
        for z in zs:
            at = z + SITES
            mid = v1[q, at]
            square = mid * mid
            one, two = one + v0[q, at] * mid, two + square
            three = three + en[q, at] * square - mid * (v1[up, at] + v1[down, at] + v1[q, at + 1] + v1[q, at - 1])
            pair = pair + mid * pltpu.roll(mid, LANES - 1, 1)
        for j in range(SITES):
            z_at = SITES * (slot8 - 1) + j
            mine = s1[q, j]
            seam = ((col8 == 2) | (col8 == 6)) & (z_at >= min(zs)) & (z_at <= max(zs))
            rim = rim + jnp.where(seam, mine * pltpu.roll(mine, LANES - 1, 1), 0.0)
        return one, two, three - rim - jnp.where(lane8 < LANES - 1, 2.0 * pair, 0.0)

    def strips_two():
        for q in range(X):
            mine, six = strip_sum(s1, q, q + 1, (q + M - 1) % M)
            for j in range(SITES):
                g2[q, j] = edge_of(two_mul * (se[q, j] * mine[j] - six[j]) - s0[q, j])

    def level_three(x, zs):
        q, up, down = around_plane(x)
        for z in zs:
            mid, total_six = site_sum(v2, q, up, down, z, g2)
            new = three_mul * (en[q, z + SITES] * mid - total_six) - one_mul * v1[q, z + SITES]
            at = pl.ds(x * Z + z, PROBES, stride=X * Z + PAD)
            prev_ref[at, :] = mid
            cur_ref[at, :] = new

    def loop(low, high, body):
        def step(i, _):
            body(i)
            return 0
        lax.fori_loop(low, high, step, 0)

    def own_moments(zs):
        sums = (zero, zero, zero)
        for x in range(X):
            sums = moments_of(x, zs, sums)
        return sums

    def send_moments(sums):
        row = zero
        for n, acc in enumerate(sums):
            summed = jnp.broadcast_to(jnp.sum(acc, axis=1, keepdims=True), (PROBES, LANES))
            row = row + jnp.where(lane8 == PROBES * n + probe, summed, 0.0)
        moms[me] = jnp.sum(row, axis=0, keepdims=True)
        each_other(lambda to: pltpu.make_async_remote_copy(
            src_ref=moms.at[me], dst_ref=moms.at[me], send_sem=msend_sem, recv_sem=mrecv_sem,
            device_id=to, device_id_type=MESH).start())

    def unpack_own(x, _):
        unpack(x, range(Z))
        return 0

    def unpack_far(i, _):
        unpack(plane(X + i), range(Z))
        return 0

    def unpack_low(i, _):
        unpack(plane(i - 3), range(Z))
        return 0

    lax.fori_loop(0, X, unpack_own, 0)
    for copy in groups["near"]:
        copy.wait_recv()
    place_strips(0, 1)
    unpack_strips(0)
    main = range(1, Z - 1)
    loop(1, X - 1, lambda x: level_one(x, main))
    for copy in groups["far"]:
        copy.wait_recv()
    for s in range(1, nbx):
        place_strips(s, 1)
        unpack_strips(s)
    strips_one()
    if M <= X + 6:
        lax.fori_loop(0, M - X, unpack_far, 0)
    else:
        lax.fori_loop(0, 3, unpack_far, 0)
        lax.fori_loop(0, 3, unpack_low, 0)

    def ends_of(low):
        width = X - 1 - 2 * low

        def body(i):
            level_one(low + i * width, main)
        return body

    loop(0, 2, ends_of(0))
    loop(0, 2, ends_of(-1))
    middle = range(2, Z - 2)
    sums = lax.fori_loop(0, X // 2, lambda i, sums: moments_of(2 * i + 1, middle, moments_of(2 * i, middle, sums)),
                         (zero, zero, zero))
    if X % 2:
        sums = moments_of(X - 1, middle, sums)
    for n in range(3):
        accs[n] = sums[n]

    if staged:
        @pl.when(iz < last)
        def _():
            pl.semaphore_wait(above, per_plane)
            start(groups[1])

    def middle_rows():
        loop(0, X, lambda x: level_two(x, middle))
        loop(0, min(M, X + 4) - (X + 2), ends_of(-2))

    @pl.when(iz == last)
    def _():
        send_moments([accs[n] for n in range(3)])
        middle_rows()

    def side(up):
        for copy in groups[-1 if up else 1]:
            copy.wait_recv()
        outside = range(Z, Z + SITES) if up else range(-SITES, 0)
        planes(3, 3, lambda q: unpack(q, outside))
        for s in range(nbx):
            place_strips(s, 2 if up else 0)
            unpack_strips(s)
        ones = range(Z - 1, Z + 3) if up else range(-3, 1)
        twos = range(Z - 2, Z + 2) if up else range(-2, 2)
        strips_one()
        loop(0, X + 2, lambda i: level_one(i - 1, ones))
        sums = own_moments(twos)
        on = (iz != last) if up else (iz == 0)
        for n in range(3):
            accs[n] = accs[n] + jnp.where(on, sums[n], 0.0)

        if up:
            @pl.when((iz > 0) & (iz < last))
            def _():
                if staged:
                    @pl.when(iz < last - 1)
                    def _():
                        pl.semaphore_wait(entered, per_plane)
                send_moments([accs[n] for n in range(3)])

            @pl.when(iz < last)
            def _():
                middle_rows()
        else:
            @pl.when(iz == 0)
            def _():
                send_moments([accs[n] for n in range(3)])

        outer = range(Z - 1, Z) if up else range(1)
        loop(0, min(M, X + 4) - (X + 2), lambda i: level_one(i * (X + 3) - 2, outer))

    def finish(twos, zs):
        loop(0, X, lambda x: level_two(x, twos))
        loop(0, 2, lambda i: level_two(i * (X + 1) - 1, zs))
        strips_two()
        loop(0, X, lambda x: level_three(x, zs))

    bottom, top = [-1, 0, 1], [Z - 2, Z - 1, Z]

    @pl.when(iz == last)
    def _():
        side(False)
        finish(bottom, range(Z - 3))

    if staged:
        @pl.when(iz == 0)
        def _():
            pl.semaphore_wait(entered, per_plane)
            start(groups[-1])

    side(True)

    @pl.when(iz == last)
    def _():
        finish(top, range(Z - 3, Z))

    @pl.when(iz < last)
    def _():
        side(False)
        finish(bottom + top, range(Z))

    for group in groups.values():
        for copy in group:
            copy.wait_send()
    others = moms.at[pl.ds(0, total - 1)]
    pltpu.make_async_copy(others, others, msend_sem).wait()
    sites = total * X * Z * LANES
    pltpu.make_async_copy(others, others, mrecv_sem).wait()
    sums = jnp.sum(moms[...], axis=0) * (1.0 / sites)
    first = one_mul * sums
    second = two_mul * pltpu.roll(sums, LANES - PROBES, 1) - 1.0
    third = (three_mul * two_mul) * pltpu.roll(sums, LANES - 2 * PROBES, 1) - 3.0 * first
    mom_ref[...] = jnp.concatenate([first, second, third], axis=0)[:, :PROBES]


def write_out(mom_ref, prev_ref, cur_ref, mom_hbm, prev_hbm, cur_hbm, sem):
    rows = prev_hbm.shape[1]
    inner = pl.ds(0, rows)
    copies = [pltpu.make_async_copy(src, dst, sem.at[n]) for n, (src, dst) in enumerate((
        (prev_ref.at[:, inner], prev_hbm), (cur_ref.at[:, inner], cur_hbm), (mom_ref, mom_hbm)))]
    for copy in copies:
        copy.start()
    for copy in copies:
        copy.wait()


def per_device(names, sizes, probe_bits, disorder_levels):
    X, W, Y = probe_bits.shape
    if Y != LANES or STRIP * (W + 2) > LANES or X < 3:
        raise ValueError("block size")
    Z = SITES * W
    nbx = 2 if sizes["gx"] == 2 else 3
    M = nbx * X
    n_copies = (9 * nbx - 1) + 2 * (3 * nbx - 1)
    total = sizes["gx"] * sizes["gy"] * sizes["gz"]
    rows = (X, W, 1, Y)
    vmem = pl.BlockSpec(memory_space=pltpu.VMEM)
    f32, i32 = jnp.float32, jnp.int32
    tile = (PROBES, LANES)
    hbm = pl.BlockSpec(memory_space=pltpu.HBM)
    out_shape = (
        jax.ShapeDtypeStruct((3, PROBES), f32),
        jax.ShapeDtypeStruct((PROBES, X * Z, Y), f32),
        jax.ShapeDtypeStruct((PROBES, X * Z, Y), f32),
    )
    padded = jax.ShapeDtypeStruct((PROBES * (X * Z + PAD), Y), f32)
    padded_shape = (out_shape[0], padded, padded)
    results = pl.pallas_call(
        functools.partial(kernel, names, sizes),
        out_shape=padded_shape,
        in_specs=[hbm] * 4,
        out_specs=(vmem,) * 3,
        scratch_shapes=[
            pltpu.VMEM((X, W, Y), i32),
            pltpu.VMEM((X, W, Y), i32),
            pltpu.VMEM((2, M, W + 2, 1, LANES), i32),
            pltpu.VMEM((M, W + 2, 1, LANES), i32),
            pltpu.VMEM((M, W + 2, 1, LANES), i32),
            pltpu.VMEM((nbx, 3, 3, 2 * X, LANES), i32),
            pltpu.VMEM((nbx, 2 * X, LANES), i32),
            pltpu.VMEM((M, Z + 2 * SITES) + tile, f32),
            pltpu.VMEM((M, Z + 2 * SITES) + tile, f32),
            pltpu.VMEM((M, Z + 2 * SITES) + tile, f32),
            pltpu.VMEM((M, Z + 2 * SITES) + tile, f32),
            pltpu.VMEM((M, SITES) + tile, f32),
            pltpu.VMEM((M, SITES) + tile, f32),
            pltpu.VMEM((M, SITES) + tile, f32),
            pltpu.VMEM((M, SITES) + tile, f32),
            pltpu.VMEM((M, SITES) + tile, f32),
            pltpu.VMEM((nbx, 4, 2 * X, LANES), i32),
            pltpu.VMEM((3,) + tile, f32),
            pltpu.VMEM((total, 1, LANES), f32),
            pltpu.SemaphoreType.DMA((4,)),
            pltpu.SemaphoreType.DMA((n_copies,)),
            pltpu.SemaphoreType.DMA((n_copies,)),
            pltpu.SemaphoreType.DMA,
            pltpu.SemaphoreType.DMA,
            pltpu.SemaphoreType.REGULAR,
            pltpu.SemaphoreType.REGULAR,
        ],
        compiler_params=pltpu.CompilerParams(collective_id=0, has_side_effects=True,
                                             vmem_limit_bytes=40 * 1024 * 1024),
    )(*[pltpu.with_memory_space_constraint(a, pltpu.HBM) for a in (probe_bits, disorder_levels, probe_bits.reshape(rows), disorder_levels.reshape(rows))])
    moments, previous, current = pl.pallas_call(
        write_out,
        out_shape=out_shape,
        in_specs=[vmem] * 3,
        out_specs=(hbm,) * 3,
        scratch_shapes=[pltpu.SemaphoreType.DMA((3,))],
        compiler_params=pltpu.CompilerParams(vmem_limit_bytes=16 * 1024 * 1024),
    )(results[0], *[a.reshape(PROBES, X * Z + PAD, Y) for a in results[1:]])
    shape = (PROBES, X, Z, Y)
    return moments, previous.reshape(shape), current.reshape(shape)


def solution(mesh):
    placed = (P("gx", "gz", "gy"), P("gx", "gz", "gy"))
    sizes = {a: mesh.shape[a] for a in mesh.axis_names}
    return jax.shard_map(
        functools.partial(per_device, tuple(mesh.axis_names), sizes),
        mesh=mesh,
        in_specs=placed,
        out_specs=(P(), P(None, "gx", "gz", "gy"), P(None, "gx", "gz", "gy")),
        check_vma=False,
    )
```
